512 devices in a mesh: pop: 32 (over y_lo, x, core), tp: 16 (over z, y_hi).
Axes of the slice: x: 4, y: 8 (y_hi: 2, y_lo: 4; y = y_hi * 4 + y_lo), z: 8, core: 2. Of those that a mesh axis runs over, the one named last changes fastest.
Arguments:
- tokens: bfloat16 [16384, 8192], P('pop', 'tp'), may hold values from -6 to 6
- weight: bfloat16 [8192, 8192], P('pop', 'tp'), may hold values from -0.0625 to 0.0625
- left: bfloat16 [512, 8192], P('pop', 'tp'), may hold values from -0.0625 to 0.0625
- right: bfloat16 [512, 8192], P('pop', 'tp'), may hold values from -6 to 6
- target: bfloat16 [16384, 8192], P('pop', 'tp'), may hold values from -6 to 6
Outputs:
- hidden: bfloat16 [16384, 8192], P('pop', 'tp')
- update: float32 [8192, 8192], P('pop', 'tp')
The draws below stay inside these ranges and needn't reach their ends.
All inputs are finite; a program needn't handle non-finite values.
Results may differ from the reference program's by a relative error of at most 0.001.
Values may be sent and summed in bfloat16 or wider, within the bound.
A program may use at most 128 MiB of HBM per device.

```python
import jax
import jax.numpy as jnp
from jax import lax

D = 8192
LEN = 32
MEMBERS = 512
TOKENS = 16384


def block_scale(stream_key, extent, shards, least, top_value):
    def one(position, blocks):
        draws = jax.random.uniform(jax.random.fold_in(jax.random.fold_in(stream_key, 6), position), (blocks,), jnp.float32, least / len(shards), top_value / len(shards))
        return jnp.repeat(jnp.exp(draws), extent[position] // blocks).reshape((-1,) + (1,) * (len(extent) - position - 1))

    loudness = one(*shards[0])
    for cut in shards[1:]:
        loudness = loudness * one(*cut)
    return loudness


def bell_draw(key, shape, scale, limit, split=(), held_as=jnp.bfloat16):
    drawn = jax.random.normal(key, shape, jnp.float32) * scale
    if len(split) > 0:
        drawn = block_scale(key, shape, split, -0.22, 0.18) * drawn
    return jnp.clip(drawn, min=-limit, max=limit).astype(held_as)


def setup_inputs(seed: int = 0) -> dict:
    key_list = jax.random.split(jax.random.key(seed), 6)
    return {
        "tokens": bell_draw(key_list[0], (TOKENS, D), 1.0, 6.0, ((0, 32), (1, 16))),
        "weight": bell_draw(key_list[1], (D, D), D ** -0.5, 0.0625, ((0, 32), (1, 16))),
        "left": bell_draw(key_list[2], (MEMBERS, D), D ** -0.5, 0.0625, ((0, 32), (1, 16))),
        "right": bell_draw(key_list[3], (MEMBERS, D), 1.0, 6.0, ((0, 32), (1, 16))),
        "target": bell_draw(key_list[4], (TOKENS, D), 1.0, 6.0, ((0, 32), (1, 16))),
    }


sigma_scale = 0.5
epsilon = 1e-06

def reference(tokens, weight, left, right, target):
    base = jnp.dot(tokens, weight, preferred_element_type=jnp.float32)
    grouped = tokens.astype(jnp.float32).reshape(MEMBERS, LEN, D)
    scores = jnp.einsum('mld,md->ml', grouped, left.astype(jnp.float32))
    full = base.reshape(MEMBERS, LEN, D) + sigma_scale * scores[:, :, None] * right.astype(jnp.float32)[:, None, :] + grouped
    hidden = full.astype(jnp.bfloat16).reshape(TOKENS, D)
    differ = full - target.astype(jnp.float32).reshape(MEMBERS, LEN, D)
    losses = lax.optimization_barrier(jnp.sum(differ * differ, axis=(1, 2))) / (LEN * D)
    mean = jnp.mean(losses)
    spread = jnp.mean(losses * losses) - mean * mean
    fitness = -(losses - mean) / jnp.sqrt(spread + epsilon)
    weighted = fitness[:, None] * left.astype(jnp.float32)
    update = jnp.dot(weighted.T, right.astype(jnp.float32), precision=lax.Precision.HIGHEST) / (MEMBERS * sigma_scale)
    return (hidden, update)
```

```python
import functools

import jax
import jax.numpy as jnp
from jax import lax
from jax.experimental import pallas as pl
from jax.experimental.pallas import tpu as pltpu
from jax.sharding import PartitionSpec as P

D = 8192
LEN = 32
MEMBERS = 512

sigma_scale = 0.5
epsilon = 1e-06

MESH = pl.DeviceIdType.MESH
NX, NY, NYL, NZ = 4, 8, 4, 8
NPOP, NTP = 32, 16
ROWS = 512
COLS = 512
KB = 256
MEM = 16
TB = ROWS + MEM
WB = KB + MEM
HALF = 256
WHALF = 128


def kernel(
    tok_hbm, w_hbm, left_hbm, right_hbm, tgt_hbm, hid_hbm, upd_hbm,
    tokbuf, wbuf, relay_a, relay_b, acc, sc, tgt, hid, leftbuf, left_t, upd, loss1, loss2,
    loc, zs, zr, ys, yr, xs, xr, fs, fr, cs, cr, rs, rr, qs, qr, las, lar, t1s, t1r, t2s, t2r,
):
    p = lax.axis_index("pop")
    t = lax.axis_index("tp")
    core = p % 2
    x = (p // 2) % NX
    yl = p // (2 * NX)
    z = t // 2
    yh = t % 2
    y = yh * NYL + yl

    def pop_of(yl_, x_, c_):
        return (yl_ * NX + x_) * 2 + c_

    def at_y(y_):
        y_ = y_ % NY
        return (pop_of(y_ % NYL, x, core), z * 2 + y_ // NYL)

    def at_x(x_):
        return (pop_of(yl, x_ % NX, core), t)

    def at_z(z_):
        return (p, (z_ % NZ) * 2 + yh)

    other_core = (pop_of(yl, x, 1 - core), t)
    t_mate = z * 2 + (1 - yh)

    loads = [
        pltpu.make_async_copy(tok_hbm, tokbuf.at[t, pl.ds(0, ROWS)], loc.at[0]),
        pltpu.make_async_copy(left_hbm, tokbuf.at[t, pl.ds(ROWS, MEM)], loc.at[1]),
        pltpu.make_async_copy(w_hbm, wbuf.at[p, pl.ds(0, KB)], loc.at[2]),
        pltpu.make_async_copy(right_hbm, wbuf.at[p, pl.ds(KB, MEM)], loc.at[3]),
        pltpu.make_async_copy(tgt_hbm, tgt, loc.at[4]),
    ]
    for c in loads:
        c.start()

    barrier = pltpu.get_barrier_semaphore()
    near = [at_y(y + k + NY) for k in (1, -1, 2, -2, 3, -3)]
    near += [at_x(x + 1), at_x(x + NX - 1), at_z(z + 1), at_z(z + NZ - 1), other_core]
    for d in near:
        pl.semaphore_signal(barrier, inc=1, device_id=d, device_id_type=MESH)
    acc[...] = jnp.zeros_like(acc)
    sc[...] = jnp.zeros_like(sc)
    pl.semaphore_wait(barrier, len(near))

    def remote(src, dst, s, r, dev):
        return pltpu.make_async_remote_copy(
            src_ref=src, dst_ref=dst, send_sem=s, recv_sem=r, device_id=dev, device_id_type=MESH
        )

    sent = []

    def go(c):
        c.start()
        sent.append(c)

    def chunk(block, c):
        return tokbuf.at[block, pl.ds(0, HALF)] if c == 0 else tokbuf.at[block, pl.ds(HALF, TB - HALF)]

    def zcopy(ring, way, j):
        c = j % 2 if way == 0 else 1 - j % 2
        dist = j // 2
        src_z = z + NZ - dist if way == 0 else z + dist
        block = (src_z % NZ) * 2 + (yh if ring == 0 else 1 - yh)
        ref = chunk(block, c)
        dev = at_z(z + 1) if way == 0 else at_z(z + NZ - 1)
        return remote(ref, ref, zs.at[way, ring, j], zr.at[way, ring, j], dev)

    def zwait(ring, way, j):
        c = j % 2 if way == 0 else 1 - j % 2
        dist = j // 2 + 1
        src_z = z + NZ - dist if way == 0 else z + dist
        block = (src_z % NZ) * 2 + (yh if ring == 0 else 1 - yh)
        ref = chunk(block, c)
        dev = at_z(z + NZ - 1) if way == 0 else at_z(z + 1)
        remote(ref, ref, zs.at[way, ring, j], zr.at[way, ring, j], dev).wait_recv()

    def zevent(ring, j):
        for way in (0, 1):
            zwait(ring, way, j)
            if j + 2 < 7:
                go(zcopy(ring, way, j + 2))

    def wblock(k, dx):
        return pop_of((yl + NYL - k) % NYL, (x + dx + NX) % NX, core)

    def ysend(k):
        ref = wbuf.at[p]
        go(remote(ref, ref, ys.at[k - 1], yr.at[k - 1], (pop_of((yl + k) % NYL, x, core), t)))

    def ywait(k):
        ref = wbuf.at[wblock(k, 0)]
        remote(ref, ref, ys.at[k - 1], yr.at[k - 1], other_core).wait_recv()

    def csend(k, dx):
        ref = wbuf.at[wblock(k, dx)]
        i = k * NX + (dx % NX)
        go(remote(ref, ref, cs.at[i], cr.at[i], other_core))

    def cwait(k, dx):
        ref = wbuf.at[pop_of((yl + NYL - k) % NYL, (x + dx + NX) % NX, 1 - core)]
        i = k * NX + (dx % NX)
        remote(ref, ref, cs.at[i], cr.at[i], other_core).wait_recv()

    def xsend(k):
        ref = wbuf.at[wblock(k, 0)]
        go(remote(ref, ref, xs.at[0, k], xr.at[0, k], at_x(x + 1)))
        go(remote(ref, ref, xs.at[1, k], xr.at[1, k], at_x(x + NX - 1)))
        csend(k, 0)

    lo, hi = pl.ds(0, WHALF), pl.ds(WHALF, WB - WHALF)

    def xwait(k):
        for way, dx, part, dev in ((0, -1, lo, at_x(x + 1)), (1, 1, hi, at_x(x + NX - 1))):
            ref = wbuf.at[wblock(k, dx)]
            remote(ref, ref, xs.at[way, k], xr.at[way, k], other_core).wait_recv()
            ref = wbuf.at[wblock(k, dx), part]
            go(remote(ref, ref, fs.at[way, k], fr.at[way, k], dev))
            csend(k, dx)

    def fwait(k):
        for way, part in ((0, lo), (1, hi)):
            ref = wbuf.at[wblock(k, 2), part]
            remote(ref, ref, fs.at[way, k], fr.at[way, k], other_core).wait_recv()
        csend(k, 2)

    def left_copy(block, c, src_p):
        ref = tokbuf.at[block, pl.ds(ROWS, MEM), pl.ds(c * KB, KB)]
        to = 2 * block + c
        return remote(ref, leftbuf.at[src_p], las.at[to], lar.at[src_p], (to, t))

    def product(j, _):
        ring, i = j // NZ, j % NZ
        odd = i % 2
        off = (odd * ((i + 1) // 2) + (1 - odd) * (NZ - i // 2)) % NZ
        block = ((z + off) % NZ) * 2 + (yh + ring) % 2
        for c in (0, 1):
            to = 2 * block + c

            @pl.when(to != p)
            def _():
                left_copy(block, c, p).start()

            @pl.when(to == p)
            def _():
                leftbuf[p] = tokbuf[block, pl.ds(ROWS, MEM), pl.ds(c * KB, KB)]

        a = tokbuf[block, pl.ds(0, ROWS)]
        acc[...] += jnp.dot(
            a[:, :KB], wbuf[2 * block, pl.ds(0, KB)], preferred_element_type=jnp.float32
        ) + jnp.dot(a[:, KB:], wbuf[2 * block + 1, pl.ds(0, KB)], preferred_element_type=jnp.float32)
        sc[...] += lax.dot_general(
            a, tokbuf[block, pl.ds(ROWS, MEM)], (((1,), (1,)), ((), ())), preferred_element_type=jnp.float32
        )
        return 0

    def products(first, last):
        lax.fori_loop(first, last, product, 0)

    loads[0].wait()
    loads[1].wait()
    first, second = chunk(t, 0), chunk(t, 1)
    go(remote(first, relay_a, rs.at[0], rr.at[0], at_y(y + 1)))
    go(remote(second, relay_b, rs.at[1], rr.at[1], at_y(y + NY - 1)))
    for j in (0, 1):
        for way in (0, 1):
            go(zcopy(0, way, j))
    loads[2].wait()
    loads[3].wait()
    xsend(0)
    for k in (1, 3, 2):
        ysend(k)

    zevent(0, 0)
    for way, buf, c, step in ((0, relay_a, 0, 3), (1, relay_b, 1, NY - 3)):
        remote(buf, buf, rs.at[way], rr.at[way], other_core).wait_recv()
        y_to = (y + step) % NY
        y_from = (y_to + NYL) % NY
        go(remote(buf, chunk(z * 2 + y_from // NYL, c), qs.at[way], qr.at[way], at_y(y_to)))
    xwait(0)
    zevent(0, 1)
    fwait(0)
    zevent(0, 2)
    zevent(0, 3)
    for k in (1, 3):
        ywait(k)
        xsend(k)
    zevent(0, 4)
    zevent(0, 5)
    for way, c in ((0, 0), (1, 1)):
        ref = chunk(t_mate, c)
        remote(ref, ref, qs.at[way], qr.at[way], other_core).wait_recv()
    for j in (0, 1):
        for way in (0, 1):
            go(zcopy(1, way, j))
    xwait(1)
    xwait(3)
    zevent(0, 6)
    ywait(2)
    xsend(2)
    fwait(1)
    fwait(3)
    zevent(1, 0)
    xwait(2)
    zevent(1, 1)
    fwait(2)
    for k in range(NYL):
        for dx in (0, -1, 1, 2):
            cwait(k, dx)
    products(0, 4)
    zevent(1, 2)
    products(4, 8)
    zevent(1, 3)
    products(8, 11)
    zevent(1, 4)
    products(11, 13)
    zevent(1, 5)
    products(13, 15)
    loads[4].wait()
    zevent(1, 6)
    products(15, 16)

    right_rows = wbuf[p, pl.ds(KB, MEM)].astype(jnp.float32)
    lane = lax.broadcasted_iota(jnp.int32, (LEN, MEM), 1)
    place = lax.broadcasted_iota(jnp.int32, (8, 128), 0) * 128 + lax.broadcasted_iota(jnp.int32, (8, 128), 1)
    mine = jnp.zeros((8, 128), jnp.float32)
    for m in range(MEM):
        rows = pl.ds(m * LEN, LEN)
        s = jnp.sum(jnp.where(lane == m, sc[rows, :], 0.0), axis=1, keepdims=True)
        full = acc[rows, :] + (sigma_scale * s) * right_rows[m : m + 1, :] + tokbuf[t, rows].astype(jnp.float32)
        hid[rows, :] = full.astype(jnp.bfloat16)
        differ = full - tgt[rows, :].astype(jnp.float32)
        total = jnp.sum(jnp.sum(differ * differ, axis=0, keepdims=True), axis=1, keepdims=True)
        mine = mine + jnp.where(place == p * MEM + m, total, 0.0)
    loss1[t] = mine

    def tp_copy(k):
        return remote(loss1.at[t], loss1.at[t], t1s.at[k], t1r.at[k], (p, (t + k) % NTP))

    def tp_wait(k, _):
        ref = loss1.at[(t + NTP - k) % NTP]
        remote(ref, ref, t1s.at[k], t1r.at[k], other_core).wait_recv()
        return 0

    def pop_copy(k):
        return remote(loss2.at[p], loss2.at[p], t2s.at[k], t2r.at[k], ((p + k) % NPOP, t))

    def pop_wait(k, _):
        ref = loss2.at[(p + NPOP - k) % NPOP]
        remote(ref, ref, t2s.at[k], t2r.at[k], other_core).wait_recv()
        return 0

    def started(copy):
        def body(k, _):
            copy(k).start()
            return 0
        return body

    lax.fori_loop(1, NTP, started(tp_copy), 0)
    hid_out = pltpu.make_async_copy(hid, hid_hbm, loc.at[5])
    hid_out.start()

    def left_wait(k, _):
        src_p = (p + NPOP - k) % NPOP
        ref = leftbuf.at[src_p]
        remote(ref, ref, las.at[src_p], lar.at[src_p], other_core).wait_recv()
        return 0

    lax.fori_loop(1, NPOP, left_wait, 0)
    left_t[...] = leftbuf[...].reshape(MEMBERS, KB).astype(jnp.float32).T

    lax.fori_loop(1, NTP, tp_wait, 0)
    loss2[p] = jnp.sum(loss1[...], axis=0)
    lax.fori_loop(1, NPOP, started(pop_copy), 0)
    lax.fori_loop(1, NPOP, pop_wait, 0)
    losses = jnp.sum(loss2[...], axis=0) / (LEN * D)
    mean = jnp.sum(losses) / MEMBERS
    spread = jnp.sum(losses * losses) / MEMBERS - mean * mean
    fitness = -(losses - mean) / jnp.sqrt(jnp.full((8, 128), spread + epsilon, jnp.float32))

    total = None
    for q in range(4):
        part = left_t[:, q * 128 : (q + 1) * 128] * fitness[q : q + 1, :]
        r = wbuf[pl.ds(q * 8, 8), pl.ds(KB, MEM)].reshape(128, COLS)
        b1 = part.astype(jnp.bfloat16)
        rest = part - b1.astype(jnp.float32)
        b2 = rest.astype(jnp.bfloat16)
        b3 = (rest - b2.astype(jnp.float32)).astype(jnp.bfloat16)
        d = (
            jnp.dot(b3, r, preferred_element_type=jnp.float32)
            + jnp.dot(b2, r, preferred_element_type=jnp.float32)
            + jnp.dot(b1, r, preferred_element_type=jnp.float32)
        )
        total = d if total is None else total + d
    upd[...] = total * (1.0 / (MEMBERS * sigma_scale))
    upd_out = pltpu.make_async_copy(upd, upd_hbm, loc.at[6])
    upd_out.start()

    for c in sent:
        c.wait_send()

    def left_sent(k, _):
        to = (p + k) % NPOP
        ref = tokbuf.at[to // 2, pl.ds(ROWS, MEM), pl.ds(0, KB)]
        remote(ref, leftbuf.at[p], las.at[to], lar.at[p], (to, t)).wait_send()
        return 0

    def tp_sent(k, _):
        tp_copy(k).wait_send()
        return 0

    def pop_sent(k, _):
        pop_copy(k).wait_send()
        return 0

    lax.fori_loop(1, NPOP, left_sent, 0)
    lax.fori_loop(1, NTP, tp_sent, 0)
    lax.fori_loop(1, NPOP, pop_sent, 0)
    hid_out.wait()
    upd_out.wait()


def per_device(tokens, weight, left, right, target):
    dma = pltpu.SemaphoreType.DMA
    bf, f32 = jnp.bfloat16, jnp.float32
    return pl.pallas_call(
        kernel,
        out_shape=(jax.ShapeDtypeStruct((ROWS, COLS), bf), jax.ShapeDtypeStruct((KB, COLS), f32)),
        in_specs=[pl.BlockSpec(memory_space=pl.ANY)] * 5,
        out_specs=(pl.BlockSpec(memory_space=pl.ANY), pl.BlockSpec(memory_space=pl.ANY)),
        scratch_shapes=[
            pltpu.VMEM((NTP, TB, COLS), bf),
            pltpu.VMEM((NPOP, WB, COLS), bf),
            pltpu.VMEM((HALF, COLS), bf),
            pltpu.VMEM((TB - HALF, COLS), bf),
            pltpu.VMEM((ROWS, COLS), f32),
            pltpu.VMEM((ROWS, MEM), f32),
            pltpu.VMEM((ROWS, COLS), bf),
            pltpu.VMEM((ROWS, COLS), bf),
            pltpu.VMEM((NPOP, MEM, KB), bf),
            pltpu.VMEM((KB, MEMBERS), f32),
            pltpu.VMEM((KB, COLS), f32),
            pltpu.VMEM((NTP, 8, 128), f32),
            pltpu.VMEM((NPOP, 8, 128), f32),
            dma((7,)),
            dma((2, 2, 7)), dma((2, 2, 7)),
            dma((3,)), dma((3,)),
            dma((2, 4)), dma((2, 4)),
            dma((2, 4)), dma((2, 4)),
            dma((16,)), dma((16,)),
            dma((2,)), dma((2,)),
            dma((2,)), dma((2,)),
            dma((NPOP,)), dma((NPOP,)),
            dma((NTP,)), dma((NTP,)),
            dma((NPOP,)), dma((NPOP,)),
        ],
        compiler_params=pltpu.CompilerParams(
            collective_id=0, has_side_effects=True, vmem_limit_bytes=56 * 1024 * 1024
        ),
    )(tokens, weight, left, right, target)


def solution(mesh):
    return jax.shard_map(
        per_device,
        mesh=mesh,
        in_specs=(P("pop", "tp"), P("pop", "tp"), P("pop", "tp"), P("pop", "tp"), P("pop", "tp")),
        out_specs=(P("pop", "tp"), P("pop", "tp")),
        check_vma=False,
    )
```

```python
import functools

import jax
import jax.numpy as jnp
from jax import lax
from jax.experimental import pallas as pl
from jax.experimental.pallas import tpu as pltpu
from jax.sharding import PartitionSpec as P

D = 8192
LEN = 32
MEMBERS = 512

sigma_scale = 0.5
epsilon = 1e-06

MESH = pl.DeviceIdType.MESH
NX, NY, NYL, NZ = 4, 8, 4, 8
NPOP, NTP = 32, 16
ROWS = 512
COLS = 512
KB = 256
MEM = 16
TB = ROWS + MEM
WB = KB + MEM
HALF = 256
WHALF = 128


def kernel(
    tok_hbm, w_hbm, left_hbm, right_hbm, tgt_hbm, hid, upd,
    tokbuf, wbuf, relay_a, relay_b, acc, sc, tgt, leftbuf, left_t, loss1, loss2,
    loc, z_sent, zr, t_sent, rr, mr, y_sent, w_sent, yr, xr, fr, cr, small_sent, small_got,
):
    p = lax.axis_index("pop")
    t = lax.axis_index("tp")
    core = p % 2
    x = (p // 2) % NX
    yl = p // (2 * NX)
    z = t // 2
    yh = t % 2
    y = yh * NYL + yl

    def pop_of(yl_, x_, c_):
        return (yl_ * NX + x_) * 2 + c_

    def at_yx(y_, x_):
        return (pop_of(y_ % NYL, x_, core), z * 2 + y_ // NYL)

    def at_y(y_):
        return at_yx(y_ % NY, x)

    def at_x(x_):
        return (pop_of(yl, x_ % NX, core), t)

    def at_z(z_):
        return (p, (z_ % NZ) * 2 + yh)

    other_core = (pop_of(yl, x, 1 - core), t)

    middle = (yl == 1) | (yl == 2)
    edge = jnp.logical_not(middle)

    barrier = pltpu.get_barrier_semaphore()
    near = [at_y(y + k + NY) for k in (1, -1, 3, -3)]
    near += [at_x(x + 1), at_x(x + NX - 1), at_z(z + 1), at_z(z + NZ - 1), other_core]
    for d in near:
        pl.semaphore_signal(barrier, inc=1, device_id=d, device_id_type=MESH)
    loads = [
        pltpu.make_async_copy(tok_hbm, tokbuf.at[t, pl.ds(0, ROWS)], loc.at[0]),
        pltpu.make_async_copy(left_hbm, tokbuf.at[t, pl.ds(ROWS, MEM)], loc.at[1]),
        pltpu.make_async_copy(w_hbm, wbuf.at[p, pl.ds(0, KB)], loc.at[2]),
        pltpu.make_async_copy(right_hbm, wbuf.at[p, pl.ds(KB, MEM)], loc.at[3]),
        pltpu.make_async_copy(tgt_hbm, tgt, loc.at[4]),
    ]
    for c in loads:
        c.start()

    acc[...] = jnp.zeros_like(acc)
    sc[...] = jnp.zeros_like(sc)
    pl.semaphore_wait(barrier, len(near))

    def remote(src, dst, s, r, dev):
        return pltpu.make_async_remote_copy(
            src_ref=src, dst_ref=dst, send_sem=s, recv_sem=r, device_id=dev, device_id_type=MESH
        )

    def got(ref, sem):
        remote(ref, ref, z_sent, sem, other_core).wait_recv()

    def left_device(ref, sem):
        remote(ref, ref, sem, mr.at[0], other_core).wait_send()

    def chunk(block, c):
        return tokbuf.at[block, pl.ds(0, HALF)] if c == 0 else tokbuf.at[block, pl.ds(HALF, TB - HALF)]

    def ring_chunk(ring, way, j, dist):
        c = j % 2 if way == 0 else 1 - j % 2
        src_z = z + NZ - dist if way == 0 else z + dist
        return chunk((src_z % NZ) * 2 + (yh if ring == 0 else 1 - yh), c)

    def zsend(ring, j):
        for way in (0, 1):
            zsend_way(ring, way, j)

    def zsend_way(ring, way, j):
        ref = ring_chunk(ring, way, j, j // 2)
        dev = at_z(z + 1) if way == 0 else at_z(z + NZ - 1)
        remote(ref, ref, z_sent, zr.at[way, ring, j], dev).start()

    def zevent(ring, j):
        for way in (0, 1):
            got(ring_chunk(ring, way, j, j // 2 + 1), zr.at[way, ring, j])
            if j + 2 < 7 - ring:
                zsend_way(ring, way, j + 2)

    def to_relay(n, block):
        first, second = chunk(block, 0), chunk(block, 1)
        remote(first, relay_a.at[n], t_sent, rr.at[n, 0], at_y(y + 1)).start()
        remote(second, relay_b.at[n], t_sent, rr.at[n, 1], at_y(y + NY - 1)).start()

    def from_relay(n, src_z):
        for way, buf, step in ((0, relay_a.at[n], 3), (1, relay_b.at[n], NY - 3)):
            got(buf, rr.at[n, way])
            y_to = (y + step) % NY
            y_from = (y_to + NYL) % NY
            dst = chunk((src_z % NZ) * 2 + y_from // NYL, way)
            remote(buf, dst, t_sent, mr.at[n], at_y(y_to)).start()

    def mate(n, src_z):
        got(tokbuf.at[(src_z % NZ) * 2 + (1 - yh)], mr.at[n])

    near_y = yl - 1 + 2 * ((3 - yl) // 3)
    far_y = 3 * ((3 - yl) // 2)
    group = (yl, near_y, 6 - yl - near_y - far_y, far_y)

    def wblock(k, dx):
        return wbuf.at[pop_of(group[k], (x + dx + NX) % NX, core)]

    def csend(k, dx):
        ref = wblock(k, dx)
        remote(ref, ref, w_sent, cr.at[k], other_core).start()

    def xsend(k):
        ref = wblock(k, 0)
        remote(ref, ref, w_sent, xr.at[0, k], at_x(x + 1)).start()
        remote(ref, ref, w_sent, xr.at[1, k], at_x(x + NX - 1)).start()
        csend(k, 0)

    def ysend(k, up, down):
        ref = wblock(k, 0)

        @pl.when(up)
        def _():
            remote(ref, ref, y_sent, yr.at[group[k]], (pop_of((yl + 1) % NYL, x, core), t)).start()

        @pl.when(down)
        def _():
            remote(ref, ref, y_sent, yr.at[group[k]], (pop_of((yl + NYL - 1) % NYL, x, core), t)).start()

    def yown():
        ysend(0, yl < NYL - 1, yl > 0)

    def ywait(k):
        src = group[k]
        got(wblock(k, 0), yr.at[src])
        ysend(k, (src < yl) & (yl < NYL - 1), (src > yl) & (yl > 0))
        xsend(k)

    lo, hi = pl.ds(0, WHALF), pl.ds(WHALF, WB - WHALF)

    def xwait(k):
        for way, dx, part, dev in ((0, -1, lo, at_x(x + 1)), (1, 1, hi, at_x(x + NX - 1))):
            got(wblock(k, dx), xr.at[way, k])
            ref = wblock(k, dx).at[part]
            remote(ref, ref, w_sent, fr.at[k], dev).start()
            csend(k, dx)

    def fwait(k):
        got(wblock(k, 2), fr.at[k])
        csend(k, 2)

    def base_rows(block, rows):
        a = tokbuf[block, rows]
        acc[rows, :] += jnp.dot(
            a[:, :KB], wbuf[2 * block, pl.ds(0, KB)], preferred_element_type=jnp.float32
        ) + jnp.dot(a[:, KB:], wbuf[2 * block + 1, pl.ds(0, KB)], preferred_element_type=jnp.float32)

    def score_rows(block, rows):
        sc[rows, :] += lax.dot_general(
            tokbuf[block, rows], tokbuf[block, pl.ds(ROWS, MEM)], (((1,), (1,)), ((), ())),
            preferred_element_type=jnp.float32,
        )

    def left_rows(block):
        for c in (0, 1):
            to = 2 * block + c
            ref = tokbuf.at[block, pl.ds(ROWS, MEM), pl.ds(c * KB, KB)]

            @pl.when(to != p)
            def _():
                remote(ref, leftbuf.at[p], small_sent.at[0], small_got.at[0], (to, t)).start()

            @pl.when(to == p)
            def _():
                leftbuf[p] = ref[...]

    every = pl.ds(0, ROWS)

    def product(block):
        left_rows(block)
        base_rows(block, every)
        score_rows(block, every)

    def at_offset(ring, off):
        return ((z + off) % NZ) * 2 + (yh + ring) % 2

    def group_products(k):
        got(wbuf.at[pl.ds(0, NX)], cr.at[k])

        def body(i, _):
            product((group[k] * 2 + i) * 2 + yh)
            return 0

        lax.fori_loop(0, 2, body, 0)

    def ring_products(first, last):
        def body(i, _):
            odd = i % 2
            product(at_offset(1, (odd * ((i + 1) // 2) + (1 - odd) * (NZ - i // 2)) % NZ))
            return 0

        lax.fori_loop(first, last, body, 0)

    top, low = pl.ds(0, HALF), pl.ds(HALF, ROWS - HALF)

    loads[0].wait()
    loads[1].wait()
    zsend(0, 0)
    zsend(0, 1)
    loads[2].wait()
    loads[3].wait()
    yown()
    to_relay(0, t)
    xsend(0)

    middle = (yl == 1) | (yl == 2)
    edge = jnp.logical_not(middle)

    zevent(0, 0)
    ywait(1)
    pl.when(middle)(functools.partial(ywait, 2))
    xwait(0)
    zevent(0, 1)
    from_relay(0, z)
    zevent(0, 2)
    pl.when(middle)(functools.partial(ywait, 3))
    pl.when(edge)(functools.partial(ywait, 2))
    zevent(0, 3)
    xwait(1)
    fwait(0)
    zevent(0, 4)
    zevent(0, 5)
    mate(0, z)
    zsend(1, 0)
    zsend(1, 1)
    xwait(2)
    zevent(0, 6)
    to_relay(1, at_offset(0, 4))
    pl.when(edge)(functools.partial(ywait, 3))
    fwait(1)
    zevent(1, 0)
    fwait(2)
    group_products(0)
    zevent(1, 1)
    from_relay(1, z + 4)
    xwait(3)
    group_products(1)
    zevent(1, 2)
    group_products(2)
    fwait(3)
    zevent(1, 3)
    group_products(3)
    ring_products(0, 3)
    zevent(1, 4)
    ring_products(3, 5)
    before, after = at_offset(1, NZ - 3), at_offset(1, 3)
    base_rows(before, top)
    base_rows(after, low)
    score_rows(after, low)
    loads[4].wait()
    mate(1, z + 4)
    product(at_offset(1, 4))
    zevent(1, 5)
    base_rows(before, low)
    base_rows(after, top)
    score_rows(before, every)
    score_rows(after, top)
    left_rows(before)
    left_rows(after)

    right_rows = wbuf[p, pl.ds(KB, MEM)].astype(jnp.float32)
    lane = lax.broadcasted_iota(jnp.int32, (LEN, MEM), 1)
    place = lax.broadcasted_iota(jnp.int32, (1, 128), 1)
    mine = jnp.zeros((1, 128), jnp.float32)
    for m in range(MEM):
        rows = pl.ds(m * LEN, LEN)
        s = jnp.sum(jnp.where(lane == m, sc[rows, :], 0.0), axis=1, keepdims=True)
        full = acc[rows, :] + (sigma_scale * s) * right_rows[m : m + 1, :] + tokbuf[t, rows].astype(jnp.float32)
        hid[rows, :] = full.astype(jnp.bfloat16)
        differ = full - tgt[rows, :].astype(jnp.float32)
        total = jnp.sum(jnp.sum(differ * differ, axis=0, keepdims=True), axis=1, keepdims=True)
        mine = mine + jnp.where(place == (p % 8) * MEM + m, total, 0.0)
    loss1[z * 2 + core] = mine

    ref = loss1.at[z * 2 + core]
    for dz in (4, 3, 5, 2, 6, 1, 7, 0):
        for dc in (1, 0):
            if dz or dc:
                dev = (pop_of(yl, x, (core + dc) % 2), ((z + dz) % NZ) * 2 + yh)
                remote(ref, ref, small_sent.at[1], small_got.at[1], dev).start()

    got(leftbuf.at[pl.ds(0, NPOP - 1)], small_got.at[0])
    left_t[...] = leftbuf[...].reshape(MEMBERS, KB).astype(jnp.float32).T

    got(loss1.at[pl.ds(0, 15)], small_got.at[1])
    row = loss1[0]
    for i in range(1, 16):
        row = row + loss1[i]
    loss2[y * NX + x] = row
    ref = loss2.at[y * NX + x]
    for dy in (4, 3, 5, 2, 6, 1, 7, 0):
        for dx in (2, 1, 3, 0):
            if dy or dx:
                remote(ref, ref, small_sent.at[2], small_got.at[2], at_yx((y + dy) % NY, (x + dx) % NX)).start()
    got(loss2.at[pl.ds(0, 31)], small_got.at[2])

    losses = []
    for q in range(NYL):
        row = loss2[q * NX]
        for i in range(1, NX):
            row = row + loss2[q * NX + i]
        for i in range(NX):
            row = row + loss2[(NYL + q) * NX + i]
        losses.append(row / (LEN * D))
    mean = jnp.sum(losses[0] + losses[1] + losses[2] + losses[3]) / MEMBERS
    squares = [row * row for row in losses]
    spread = jnp.sum(squares[0] + squares[1] + squares[2] + squares[3]) / MEMBERS - mean * mean
    root = jnp.sqrt(jnp.full((1, 128), spread + epsilon, jnp.float32))

    fitness = jnp.concatenate([-(row - mean) / root for row in losses], axis=1)
    weighted = left_t[...] * fitness
    b1 = weighted.astype(jnp.bfloat16)
    b2 = (weighted - b1.astype(jnp.float32)).astype(jnp.bfloat16)
    r = wbuf[:, pl.ds(KB, MEM)].reshape(MEMBERS, COLS)
    total = jnp.dot(b2, r, preferred_element_type=jnp.float32) + jnp.dot(b1, r, preferred_element_type=jnp.float32)
    upd[...] = total * (1.0 / (MEMBERS * sigma_scale))

    left_device(tokbuf.at[pl.ds(0, 13)], z_sent)
    left_device(tokbuf.at[pl.ds(0, 4)], t_sent)
    left_device(wbuf.at[pl.ds(0, 28)], w_sent)
    @pl.when(middle)
    def _():
        left_device(wbuf.at[pl.ds(0, 5)], y_sent)

    @pl.when(edge)
    def _():
        left_device(wbuf.at[0], y_sent)

    left_device(leftbuf.at[pl.ds(0, NPOP - 1)], small_sent.at[0])
    left_device(loss1.at[pl.ds(0, 15)], small_sent.at[1])
    left_device(loss2.at[pl.ds(0, 31)], small_sent.at[2])


def write_out(hid, upd, hid_hbm, upd_hbm, sem):
    copies = [pltpu.make_async_copy(hid, hid_hbm, sem.at[0]), pltpu.make_async_copy(upd, upd_hbm, sem.at[1])]
    for c in copies:
        c.start()
    for c in copies:
        c.wait()


def per_device(tokens, weight, left, right, target):
    dma = pltpu.SemaphoreType.DMA
    bf, f32 = jnp.bfloat16, jnp.float32
    hidden, update = pl.pallas_call(
        kernel,
        out_shape=(pltpu.VMEM((ROWS, COLS), bf), pltpu.VMEM((KB, COLS), f32)),
        in_specs=[pl.BlockSpec(memory_space=pl.ANY)] * 5,
        out_specs=(pl.BlockSpec(memory_space=pltpu.VMEM), pl.BlockSpec(memory_space=pltpu.VMEM)),
        scratch_shapes=[
            pltpu.VMEM((NTP, TB, COLS), bf),
            pltpu.VMEM((NPOP, WB, COLS), bf),
            pltpu.VMEM((2, HALF, COLS), bf),
            pltpu.VMEM((2, TB - HALF, COLS), bf),
            pltpu.VMEM((ROWS, COLS), f32),
            pltpu.VMEM((ROWS, MEM), f32),
            pltpu.VMEM((ROWS, COLS), bf),
            pltpu.VMEM((NPOP, MEM, KB), bf),
            pltpu.VMEM((KB, MEMBERS), f32),
            pltpu.VMEM((16, 1, 128), f32),
            pltpu.VMEM((32, 1, 128), f32),
            dma((5,)),
            dma(()), dma((2, 2, 7)),
            dma(()), dma((2, 2)), dma((2,)),
            dma(()), dma(()), dma((NYL,)), dma((2, 4)), dma((4,)), dma((4,)),
            dma((3,)), dma((3,)),
        ],
        compiler_params=pltpu.CompilerParams(
            collective_id=0, has_side_effects=True, vmem_limit_bytes=56 * 1024 * 1024
        ),
    )(tokens, weight, left, right, target)
    return pl.pallas_call(
        write_out,
        out_shape=(jax.ShapeDtypeStruct((ROWS, COLS), bf), jax.ShapeDtypeStruct((KB, COLS), f32)),
        in_specs=[pl.BlockSpec(memory_space=pl.ANY)] * 2,
        out_specs=(pl.BlockSpec(memory_space=pl.ANY), pl.BlockSpec(memory_space=pl.ANY)),
        scratch_shapes=[dma((2,))],
        compiler_params=pltpu.CompilerParams(vmem_limit_bytes=1024 * 1024),
    )(hidden, update)


def solution(mesh):
    return jax.shard_map(
        per_device,
        mesh=mesh,
        in_specs=(P("pop", "tp"), P("pop", "tp"), P("pop", "tp"), P("pop", "tp"), P("pop", "tp")),
        out_specs=(P("pop", "tp"), P("pop", "tp")),
        check_vma=False,
    )
```

```python
import functools

import jax
import jax.numpy as jnp
from jax import lax
from jax.experimental import pallas as pl
from jax.experimental.pallas import tpu as pltpu
from jax.sharding import PartitionSpec as P

D = 8192
LEN = 32
MEMBERS = 512

sigma_scale = 0.5
epsilon = 1e-06

MESH = pl.DeviceIdType.MESH
NX, NY, NYL, NZ = 4, 8, 4, 8
NPOP, NTP = 32, 16
ROWS = 512
COLS = 512
KB = 256
MEM = 16
TB = ROWS + MEM
WB = KB + MEM
QUARTER = 128
EXTRA = 32
HALF = 256
WHALF = 128


def kernel(
    tok_hbm, w_hbm, left_hbm, right_hbm, tgt_hbm, hid, upd,
    tokbuf, wbuf, relay_a, relay_b, acc, sc, tgt, leftbuf, left_t, loss1, loss2,
    loc, z_sent, zr, t_sent, rr, mr, y_sent, w_sent, yr, xr, fr, cr, small_sent, small_got,
    entered,
):
    p = lax.axis_index("pop")
    t = lax.axis_index("tp")
    core = p % 2
    x = (p // 2) % NX
    yl = p // (2 * NX)
    z = t // 2
    yh = t % 2
    y = yh * NYL + yl

    def pop_of(yl_, x_, c_):
        return (yl_ * NX + x_) * 2 + c_

    def at_yx(y_, x_):
        return (pop_of(y_ % NYL, x_, core), z * 2 + y_ // NYL)

    def at_y(y_):
        return at_yx(y_ % NY, x)

    def at_x(x_):
        return (pop_of(yl, x_ % NX, core), t)

    def at_z(z_):
        return (p, (z_ % NZ) * 2 + yh)

    other_core = (pop_of(yl, x, 1 - core), t)

    middle = (yl == 1) | (yl == 2)
    edge = jnp.logical_not(middle)

    barrier = pltpu.get_barrier_semaphore()
    near = [at_y(y + 1), at_y(y + NY - 1)]
    near += [at_x(x + 1), at_x(x + NX - 1), at_z(z + 1), at_z(z + NZ - 1), other_core]
    for d in near:
        pl.semaphore_signal(barrier, inc=1, device_id=d, device_id_type=MESH)
    loads = [
        pltpu.make_async_copy(tok_hbm, tokbuf.at[t, pl.ds(0, ROWS)], loc.at[0]),
        pltpu.make_async_copy(left_hbm, tokbuf.at[t, pl.ds(ROWS, MEM)], loc.at[1]),
        pltpu.make_async_copy(w_hbm, wbuf.at[p, pl.ds(0, KB)], loc.at[2]),
        pltpu.make_async_copy(right_hbm, wbuf.at[p, pl.ds(KB, MEM)], loc.at[3]),
        pltpu.make_async_copy(tgt_hbm, tgt, loc.at[4]),
    ]
    for c in loads:
        c.start()

    acc[...] = jnp.zeros_like(acc)
    sc[...] = jnp.zeros_like(sc)
    pl.semaphore_wait(barrier, len(near))

    def remote(src, dst, s, r, dev):
        return pltpu.make_async_remote_copy(
            src_ref=src, dst_ref=dst, send_sem=s, recv_sem=r, device_id=dev, device_id_type=MESH
        )

    def got(ref, sem):
        remote(ref, ref, z_sent.at[0], sem, other_core).wait_recv()

    def left_device(ref, sem):
        remote(ref, ref, sem, mr.at[0], other_core).wait_send()

    def chunk(block, c):
        return tokbuf.at[block, pl.ds(0, HALF)] if c == 0 else tokbuf.at[block, pl.ds(HALF, TB - HALF)]

    def ring_chunk(ring, way, j, dist):
        c = j % 2 if way == 0 else 1 - j % 2
        src_z = z + NZ - dist if way == 0 else z + dist
        block = (src_z % NZ) * 2 + (yh if ring == 0 else 1 - yh)
        if ring == 1 and j >= 5:
            c = 1 - way
            rows = QUARTER if j == 6 else QUARTER - EXTRA
            return tokbuf.at[block, pl.ds(c * HALF + (6 - j) * QUARTER, rows)]
        return chunk(block, c)

    def zsend(ring, j):
        for way in (0, 1):
            zsend_way(ring, way, j)

    def zsend_way(ring, way, j):
        ref = ring_chunk(ring, way, j, min(j // 2, 2 if ring == 1 else 3))
        dev = at_z(z + 1) if way == 0 else at_z(z + NZ - 1)
        small = ring == 1 and j >= 5
        remote(ref, ref, z_sent.at[1 if small else 0], zr.at[way, ring, j], dev).start()

    def zevent(ring, j):
        for way in (0, 1):
            got(ring_chunk(ring, way, j, min(j // 2, 2 if ring == 1 else 3) + 1), zr.at[way, ring, j])
            if j + 2 < 7 - ring:
                zsend_way(ring, way, j + 2)
            if ring == 1 and j == 3:
                zsend_way(1, way, 6)

    def pieces(n, own_yh, src_z):
        if n < 2:
            block = (src_z % NZ) * 2 + own_yh
            return chunk(block, 0), chunk(block, 1)
        after, before = ((z + 3) % NZ) * 2 + own_yh, ((z + NZ - 3) % NZ) * 2 + own_yh
        return tokbuf.at[after, pl.ds(HALF - EXTRA, EXTRA)], tokbuf.at[before, pl.ds(ROWS - EXTRA, EXTRA + MEM)]

    def relay(n):
        if n < 2:
            return relay_a.at[n], relay_b.at[n]
        return relay_a.at[n, pl.ds(0, EXTRA)], relay_b.at[n, pl.ds(0, EXTRA + MEM)]

    def to_relay(n, src_z):
        for way, ref, buf, dev in zip((0, 1), pieces(n, yh, src_z), relay(n), (at_y(y + 1), at_y(y + NY - 1))):
            remote(ref, buf, t_sent.at[n // 2], rr.at[n, way], dev).start()

    def from_relay(n, src_z):
        for way, buf, step in zip((0, 1), relay(n), (3, NY - 3)):
            got(buf, rr.at[n, way])
            y_to = (y + step) % NY
            dst = pieces(n, (y_to + NYL) % NY // NYL, src_z)[way]
            remote(buf, dst, t_sent.at[n // 2], mr.at[n], at_y(y_to)).start()

    def mate(n, src_z):
        if n < 2:
            got(tokbuf.at[(src_z % NZ) * 2 + (1 - yh)], mr.at[n])
        else:
            got(tokbuf.at[0, pl.ds(0, 2 * EXTRA + MEM)], mr.at[n])

    def tell(n):
        for way, dev in ((0, at_y(y + 1)), (1, at_y(y + NY - 1))):
            pl.semaphore_signal(entered.at[n, way], inc=1, device_id=dev, device_id_type=MESH)

    def told(n):
        for way in (0, 1):
            pl.semaphore_wait(entered.at[n, way], 1)

    near_y = yl - 1 + 2 * ((3 - yl) // 3)
    far_y = 3 * ((3 - yl) // 2)
    group = (yl, near_y, 6 - yl - near_y - far_y, far_y)

    def wblock(k, dx):
        return wbuf.at[pop_of(group[k], (x + dx + NX) % NX, core)]

    def csend(k, dx):
        ref = wblock(k, dx)
        remote(ref, ref, w_sent, cr.at[k], other_core).start()

    def xsend(k):
        ref = wblock(k, 0)
        remote(ref, ref, w_sent, xr.at[0, k], at_x(x + 1)).start()
        remote(ref, ref, w_sent, xr.at[1, k], at_x(x + NX - 1)).start()
        csend(k, 0)

    def ysend(k, up, down):
        ref = wblock(k, 0)

        @pl.when(up)
        def _():
            remote(ref, ref, y_sent, yr.at[group[k]], (pop_of((yl + 1) % NYL, x, core), t)).start()

        @pl.when(down)
        def _():
            remote(ref, ref, y_sent, yr.at[group[k]], (pop_of((yl + NYL - 1) % NYL, x, core), t)).start()

    def yown():
        ysend(0, yl < NYL - 1, yl > 0)

    def ywait(k):
        src = group[k]
        got(wblock(k, 0), yr.at[src])
        ysend(k, (src < yl) & (yl < NYL - 1), (src > yl) & (yl > 0))
        xsend(k)

    lo, hi = pl.ds(0, WHALF), pl.ds(WHALF, WB - WHALF)

    def xwait(k):
        for way, dx, part, dev in ((0, -1, lo, at_x(x + 1)), (1, 1, hi, at_x(x + NX - 1))):
            got(wblock(k, dx), xr.at[way, k])
            ref = wblock(k, dx).at[part]
            remote(ref, ref, w_sent, fr.at[k], dev).start()
            csend(k, dx)

    def fwait(k):
        got(wblock(k, 2), fr.at[k])
        csend(k, 2)

    def base_rows(block, rows):
        a = tokbuf[block, rows]
        acc[rows, :] += jnp.dot(
            a[:, :KB], wbuf[2 * block, pl.ds(0, KB)], preferred_element_type=jnp.float32
        ) + jnp.dot(a[:, KB:], wbuf[2 * block + 1, pl.ds(0, KB)], preferred_element_type=jnp.float32)

    def score_rows(block, rows):
        sc[rows, :] += lax.dot_general(
            tokbuf[block, rows], tokbuf[block, pl.ds(ROWS, MEM)], (((1,), (1,)), ((), ())),
            preferred_element_type=jnp.float32,
        )

    def left_rows(block):
        for c in (0, 1):
            to = 2 * block + c
            ref = tokbuf.at[block, pl.ds(ROWS, MEM), pl.ds(c * KB, KB)]

            @pl.when(to != p)
            def _():
                remote(ref, leftbuf.at[p], small_sent.at[0], small_got.at[0], (to, t)).start()

            @pl.when(to == p)
            def _():
                leftbuf[p] = ref[...]

    every = pl.ds(0, ROWS)

    def product(block):
        left_rows(block)
        base_rows(block, every)
        score_rows(block, every)

    def at_offset(ring, off):
        return ((z + off) % NZ) * 2 + (yh + ring) % 2

    def group_products(k):
        got(wbuf.at[pl.ds(0, NX)], cr.at[k])

        def body(i, _):
            product((group[k] * 2 + i) * 2 + yh)
            return 0

        lax.fori_loop(0, 2, body, 0)

    def ring_products(first, last):
        def body(i, _):
            odd = i % 2
            product(at_offset(1, (odd * ((i + 1) // 2) + (1 - odd) * (NZ - i // 2)) % NZ))
            return 0

        lax.fori_loop(first, last, body, 0)

    top, low = pl.ds(0, HALF), pl.ds(HALF, ROWS - HALF)

    loads[0].wait()
    loads[1].wait()
    zsend(0, 0)
    zsend(0, 1)
    tell(0)
    loads[2].wait()
    loads[3].wait()
    yown()
    to_relay(0, z)
    xsend(0)
    told(0)
    tell(1)

    zevent(0, 0)
    ywait(1)
    pl.when(middle)(functools.partial(ywait, 2))
    xwait(0)
    zevent(0, 1)
    told(1)
    from_relay(0, z)
    zevent(0, 2)
    zevent(0, 3)
    pl.when(middle)(functools.partial(ywait, 3))
    pl.when(edge)(functools.partial(ywait, 2))
    xwait(1)
    fwait(0)
    zevent(0, 4)
    zevent(0, 5)
    mate(0, z)
    zsend(1, 0)
    zsend(1, 1)
    xwait(2)
    zevent(0, 6)
    to_relay(1, z + 4)
    to_relay(2, z)
    pl.when(edge)(functools.partial(ywait, 3))
    fwait(1)
    zevent(1, 0)
    fwait(2)
    group_products(0)
    from_relay(1, z + 4)
    zevent(1, 1)
    from_relay(2, z)
    xwait(3)
    group_products(1)
    zevent(1, 2)
    group_products(2)
    fwait(3)
    zevent(1, 3)
    group_products(3)
    ring_products(0, 3)
    zevent(1, 4)
    ring_products(3, 5)
    before, after = at_offset(1, NZ - 3), at_offset(1, 3)
    base_rows(before, top)
    base_rows(after, low)
    score_rows(after, low)
    loads[4].wait()
    mate(1, z + 4)
    product(at_offset(1, 4))
    q0, q1, q2, q3 = (pl.ds(i * QUARTER, QUARTER) for i in range(4))
    right_rows = wbuf[p, pl.ds(KB, MEM)].astype(jnp.float32)
    lane = lax.broadcasted_iota(jnp.int32, (LEN, MEM), 1)
    place = lax.broadcasted_iota(jnp.int32, (1, 128), 1)

    def finish(members, mine):
        for m in members:
            rows = pl.ds(m * LEN, LEN)
            s = jnp.sum(jnp.where(lane == m, sc[rows, :], 0.0), axis=1, keepdims=True)
            full = acc[rows, :] + (sigma_scale * s) * right_rows[m : m + 1, :] + tokbuf[t, rows].astype(jnp.float32)
            hid[rows, :] = full.astype(jnp.bfloat16)
            differ = full - tgt[rows, :].astype(jnp.float32)
            total = jnp.sum(jnp.sum(differ * differ, axis=0, keepdims=True), axis=1, keepdims=True)
            mine = mine + jnp.where(place == (p % 8) * MEM + m, total, 0.0)
        return mine

    mate(2, z)
    zevent(1, 5)
    for block, seen, scored in ((before, q3, (top, q3)), (after, q1, (q1,))):
        base_rows(block, seen)
        for rows in scored:
            score_rows(block, rows)
        left_rows(block)
    per = QUARTER // LEN
    mine = finish((*range(per, 2 * per), *range(3 * per, 4 * per)), jnp.zeros((1, 128), jnp.float32))
    zevent(1, 6)
    for block, seen in ((before, q2), (after, q0)):
        base_rows(block, seen)
        score_rows(block, seen)
    loss1[z * 2 + core] = finish((*range(per), *range(2 * per, 3 * per)), mine)

    ref = loss1.at[z * 2 + core]
    for dz in (4, 3, 5, 2, 6, 1, 7, 0):
        for dc in (1, 0):
            if dz or dc:
                dev = (pop_of(yl, x, (core + dc) % 2), ((z + dz) % NZ) * 2 + yh)
                remote(ref, ref, small_sent.at[1], small_got.at[1], dev).start()

    got(leftbuf.at[pl.ds(0, NPOP - 1)], small_got.at[0])
    left_t[...] = leftbuf[...].reshape(MEMBERS, KB).astype(jnp.float32).T

    got(loss1.at[pl.ds(0, 15)], small_got.at[1])
    row = loss1[0]
    for i in range(1, 16):
        row = row + loss1[i]
    loss2[y * NX + x] = row
    ref = loss2.at[y * NX + x]
    for dy in (4, 3, 5, 2, 6, 1, 7, 0):
        for dx in (2, 1, 3, 0):
            if dy or dx:
                remote(ref, ref, small_sent.at[2], small_got.at[2], at_yx((y + dy) % NY, (x + dx) % NX)).start()
    got(loss2.at[pl.ds(0, 31)], small_got.at[2])

    losses = []
    for q in range(NYL):
        row = loss2[q * NX]
        for i in range(1, NX):
            row = row + loss2[q * NX + i]
        for i in range(NX):
            row = row + loss2[(NYL + q) * NX + i]
        losses.append(row / (LEN * D))
    mean = jnp.sum(losses[0] + losses[1] + losses[2] + losses[3]) / MEMBERS
    squares = [row * row for row in losses]
    spread = jnp.sum(squares[0] + squares[1] + squares[2] + squares[3]) / MEMBERS - mean * mean
    root = jnp.sqrt(jnp.full((1, 128), spread + epsilon, jnp.float32))

    fitness = jnp.concatenate([-(row - mean) / root for row in losses], axis=1)
    weighted = left_t[...] * fitness
    b1 = weighted.astype(jnp.bfloat16)
    b2 = (weighted - b1.astype(jnp.float32)).astype(jnp.bfloat16)
    r = wbuf[:, pl.ds(KB, MEM)].reshape(MEMBERS, COLS)
    total = jnp.dot(b2, r, preferred_element_type=jnp.float32) + jnp.dot(b1, r, preferred_element_type=jnp.float32)
    upd[...] = total * (1.0 / (MEMBERS * sigma_scale))

    left_device(tokbuf.at[pl.ds(0, 12)], z_sent.at[0])
    left_device(tokbuf.at[0, pl.ds(0, 4 * QUARTER - 2 * EXTRA)], z_sent.at[1])
    left_device(tokbuf.at[pl.ds(0, 4)], t_sent.at[0])
    left_device(tokbuf.at[0, pl.ds(0, 2 * (2 * EXTRA + MEM))], t_sent.at[1])
    left_device(wbuf.at[pl.ds(0, 28)], w_sent)
    @pl.when(middle)
    def _():
        left_device(wbuf.at[pl.ds(0, 5)], y_sent)

    @pl.when(edge)
    def _():
        left_device(wbuf.at[0], y_sent)

    left_device(leftbuf.at[pl.ds(0, NPOP - 1)], small_sent.at[0])
    left_device(loss1.at[pl.ds(0, 15)], small_sent.at[1])
    left_device(loss2.at[pl.ds(0, 31)], small_sent.at[2])


def write_out(hid, upd, hid_hbm, upd_hbm, sem):
    copies = [pltpu.make_async_copy(hid, hid_hbm, sem.at[0]), pltpu.make_async_copy(upd, upd_hbm, sem.at[1])]
    for c in copies:
        c.start()
    for c in copies:
        c.wait()


def per_device(tokens, weight, left, right, target):
    dma = pltpu.SemaphoreType.DMA
    bf, f32 = jnp.bfloat16, jnp.float32
    hidden, update = pl.pallas_call(
        kernel,
        out_shape=(pltpu.VMEM((ROWS, COLS), bf), pltpu.VMEM((KB, COLS), f32)),
        in_specs=[pl.BlockSpec(memory_space=pl.ANY)] * 5,
        out_specs=(pl.BlockSpec(memory_space=pltpu.VMEM), pl.BlockSpec(memory_space=pltpu.VMEM)),
        scratch_shapes=[
            pltpu.VMEM((NTP, TB, COLS), bf),
            pltpu.VMEM((NPOP, WB, COLS), bf),
            pltpu.VMEM((3, HALF, COLS), bf),
            pltpu.VMEM((3, TB - HALF, COLS), bf),
            pltpu.VMEM((ROWS, COLS), f32),
            pltpu.VMEM((ROWS, MEM), f32),
            pltpu.VMEM((ROWS, COLS), bf),
            pltpu.VMEM((NPOP, MEM, KB), bf),
            pltpu.VMEM((KB, MEMBERS), f32),
            pltpu.VMEM((16, 1, 128), f32),
            pltpu.VMEM((32, 1, 128), f32),
            dma((5,)),
            dma((2,)), dma((2, 2, 7)),
            dma((2,)), dma((3, 2)), dma((3,)),
            dma(()), dma(()), dma((NYL,)), dma((2, 4)), dma((4,)), dma((4,)),
            dma((3,)), dma((3,)),
            pltpu.SemaphoreType.REGULAR((2, 2)),
        ],
        compiler_params=pltpu.CompilerParams(
            collective_id=0, has_side_effects=True, vmem_limit_bytes=56 * 1024 * 1024
        ),
    )(tokens, weight, left, right, target)
    return pl.pallas_call(
        write_out,
        out_shape=(jax.ShapeDtypeStruct((ROWS, COLS), bf), jax.ShapeDtypeStruct((KB, COLS), f32)),
        in_specs=[pl.BlockSpec(memory_space=pl.ANY)] * 2,
        out_specs=(pl.BlockSpec(memory_space=pl.ANY), pl.BlockSpec(memory_space=pl.ANY)),
        scratch_shapes=[dma((2,))],
        compiler_params=pltpu.CompilerParams(vmem_limit_bytes=1024 * 1024),
    )(hidden, update)


def solution(mesh):
    return jax.shard_map(
        per_device,
        mesh=mesh,
        in_specs=(P("pop", "tp"), P("pop", "tp"), P("pop", "tp"), P("pop", "tp"), P("pop", "tp")),
        out_specs=(P("pop", "tp"), P("pop", "tp")),
        check_vma=False,
    )
```

```python
import functools

import jax
import jax.numpy as jnp
from jax import lax
from jax.experimental import pallas as pl
from jax.experimental.pallas import tpu as pltpu
from jax.sharding import PartitionSpec as P

D = 8192
LEN = 32
MEMBERS = 512

sigma_scale = 0.5
epsilon = 1e-06

MESH = pl.DeviceIdType.MESH
NX, NY, NYL, NZ = 4, 8, 4, 8
NPOP, NTP = 32, 16
ROWS = 512
COLS = 512
KB = 256
MEM = 16
TB = ROWS + MEM
WB = KB + MEM
LAST = 64
EXTRA = 32
HALF = 256
WHALF = 128


def kernel(
    tok_hbm, w_hbm, left_hbm, right_hbm, tgt_hbm, hid, upd,
    tokbuf, wbuf, relay_a, relay_b, acc, sc, tgt, leftbuf, left_t, loss1, loss2,
    loc, z_sent, zr, rr, mr, y_sent, w_sent, yr, xr, fr, cr, small_sent, small_got,
    entered,
):
    p = lax.axis_index("pop")
    t = lax.axis_index("tp")
    core = p % 2
    x = (p // 2) % NX
    yl = p // (2 * NX)
    z = t // 2
    yh = t % 2
    y = yh * NYL + yl

    def pop_of(yl_, x_, c_):
        return (yl_ * NX + x_) * 2 + c_

    def at_yx(y_, x_):
        return (pop_of(y_ % NYL, x_, core), z * 2 + y_ // NYL)

    def at_y(y_):
        return at_yx(y_ % NY, x)

    def at_x(x_):
        return (pop_of(yl, x_ % NX, core), t)

    def at_z(z_):
        return (p, (z_ % NZ) * 2 + yh)

    other_core = (pop_of(yl, x, 1 - core), t)

    middle = (yl == 1) | (yl == 2)
    edge = jnp.logical_not(middle)

    barrier = pltpu.get_barrier_semaphore()
    near = [at_z(z + 1), at_z(z + NZ - 1), at_y(y + 1), at_y(y + NY - 1), at_x(x + 1), at_x(x + NX - 1), other_core]
    for d in near:
        pl.semaphore_signal(barrier, inc=1, device_id=d, device_id_type=MESH)
    loads = [
        pltpu.make_async_copy(tok_hbm, tokbuf.at[t, pl.ds(0, ROWS)], loc.at[0]),
        pltpu.make_async_copy(left_hbm, tokbuf.at[t, pl.ds(ROWS, MEM)], loc.at[1]),
        pltpu.make_async_copy(w_hbm, wbuf.at[p, pl.ds(0, KB)], loc.at[2]),
        pltpu.make_async_copy(right_hbm, wbuf.at[p, pl.ds(KB, MEM)], loc.at[3]),
        pltpu.make_async_copy(tgt_hbm, tgt, loc.at[4]),
    ]
    for c in loads:
        c.start()

    acc[...] = jnp.zeros_like(acc)
    sc[...] = jnp.zeros_like(sc)
    pl.semaphore_wait(barrier, len(near))

    def remote(src, dst, s, r, dev):
        return pltpu.make_async_remote_copy(
            src_ref=src, dst_ref=dst, send_sem=s, recv_sem=r, device_id=dev, device_id_type=MESH
        )

    def got(ref, sem):
        remote(ref, ref, z_sent.at[0], sem, other_core).wait_recv()

    def left_device(ref, sem):
        remote(ref, ref, sem, mr.at[0], other_core).wait_send()

    def chunk(block, c):
        return tokbuf.at[block, pl.ds(0, HALF)] if c == 0 else tokbuf.at[block, pl.ds(HALF, TB - HALF)]

    def ring_chunk(ring, way, j, dist):
        c = j % 2 if way == 0 else 1 - j % 2
        src_z = z + NZ - dist if way == 0 else z + dist
        block = (src_z % NZ) * 2 + (yh if ring == 0 else 1 - yh)
        if ring == 1 and j >= 5:
            c = 1 - way
            start, rows = (0, LAST) if j == 6 else (LAST, HALF - EXTRA - LAST)
            return tokbuf.at[block, pl.ds(c * HALF + start, rows)]
        return chunk(block, c)

    def zsend(ring, j):
        for way in (0, 1):
            zsend_way(ring, way, j)

    def zsend_way(ring, way, j):
        ref = ring_chunk(ring, way, j, min(j // 2, 2 if ring == 1 else 3))
        dev = at_z(z + 1) if way == 0 else at_z(z + NZ - 1)
        small = ring == 1 and j >= 5
        remote(ref, ref, z_sent.at[1 if small else 0], zr.at[way, ring, j], dev).start()

    def zevent(ring, j):
        for way in (0, 1):
            got(ring_chunk(ring, way, j, min(j // 2, 2 if ring == 1 else 3) + 1), zr.at[way, ring, j])
            if j + 2 < 7 - ring:
                zsend_way(ring, way, j + 2)
            if ring == 1 and j == 3:
                zsend_way(1, way, 6)

    def pieces(n, own_yh, src_z):
        if n < 2:
            block = (src_z % NZ) * 2 + own_yh
            return chunk(block, 0), chunk(block, 1)
        after, before = ((z + 3) % NZ) * 2 + own_yh, ((z + NZ - 3) % NZ) * 2 + own_yh
        return tokbuf.at[after, pl.ds(HALF - EXTRA, EXTRA)], tokbuf.at[before, pl.ds(ROWS - EXTRA, EXTRA + MEM)]

    def relay(n):
        if n < 2:
            return relay_a.at[n], relay_b.at[n]
        return relay_a.at[n, pl.ds(0, EXTRA)], relay_b.at[n, pl.ds(0, EXTRA + MEM)]

    def to_relay(n, src_z):
        for way, ref, buf, dev in zip((0, 1), pieces(n, yh, src_z), relay(n), (at_y(y + 1), at_y(y + NY - 1))):
            remote(ref, buf, z_sent.at[n // 2], rr.at[n], dev).start()

    def from_relay(n, src_z):
        got(tokbuf.at[0] if n < 2 else tokbuf.at[0, pl.ds(0, 2 * EXTRA + MEM)], rr.at[n])
        for way, buf, step in zip((0, 1), relay(n), (3, NY - 3)):
            y_to = (y + step) % NY
            dst = pieces(n, (y_to + NYL) % NY // NYL, src_z)[way]
            remote(buf, dst, z_sent.at[n // 2], mr.at[n], at_y(y_to)).start()

    def mate(n, src_z):
        if n < 2:
            got(tokbuf.at[(src_z % NZ) * 2 + (1 - yh)], mr.at[n])
        else:
            got(tokbuf.at[0, pl.ds(0, 2 * EXTRA + MEM)], mr.at[n])

    def tell(n):
        for dev in (at_y(y + 1), at_y(y + NY - 1)):
            pl.semaphore_signal(entered.at[n], inc=1, device_id=dev, device_id_type=MESH)

    def told(n):
        pl.semaphore_wait(entered.at[n], 2)

    near_y = yl - 1 + 2 * ((3 - yl) // 3)
    far_y = 3 * ((3 - yl) // 2)
    group = (yl, near_y, 6 - yl - near_y - far_y, far_y)

    def wblock(k, dx):
        return wbuf.at[pop_of(group[k], (x + dx + NX) % NX, core)]

    def csend(k, dx):
        ref = wblock(k, dx)
        remote(ref, ref, w_sent, cr.at[k], other_core).start()

    def xsend(k):
        ref = wblock(k, 0)
        remote(ref, ref, w_sent, xr.at[k], at_x(x + 1)).start()
        remote(ref, ref, w_sent, xr.at[k], at_x(x + NX - 1)).start()
        csend(k, 0)

    def ysend(k, up, down):
        ref = wblock(k, 0)

        @pl.when(up)
        def _():
            remote(ref, ref, y_sent, yr.at[group[k]], (pop_of((yl + 1) % NYL, x, core), t)).start()

        @pl.when(down)
        def _():
            remote(ref, ref, y_sent, yr.at[group[k]], (pop_of((yl + NYL - 1) % NYL, x, core), t)).start()

    def yown():
        ysend(0, yl < NYL - 1, yl > 0)

    def ywait(k):
        src = group[k]
        got(wblock(k, 0), yr.at[src])
        ysend(k, (src < yl) & (yl < NYL - 1), (src > yl) & (yl > 0))
        xsend(k)

    lo, hi = pl.ds(0, WHALF), pl.ds(WHALF, WB - WHALF)

    def xwait(k):
        got(wbuf.at[pl.ds(0, 2)], xr.at[k])
        for dx, part, dev in ((-1, lo, at_x(x + 1)), (1, hi, at_x(x + NX - 1))):
            ref = wblock(k, dx).at[part]
            remote(ref, ref, w_sent, fr.at[k], dev).start()
            csend(k, dx)

    def fwait(k):
        got(wblock(k, 2), fr.at[k])
        csend(k, 2)

    def base_rows(block, rows):
        a = tokbuf[block, rows]
        acc[rows, :] += jnp.dot(
            a[:, :KB], wbuf[2 * block, pl.ds(0, KB)], preferred_element_type=jnp.float32
        ) + jnp.dot(a[:, KB:], wbuf[2 * block + 1, pl.ds(0, KB)], preferred_element_type=jnp.float32)

    def score_rows(block, rows):
        sc[rows, :] += lax.dot_general(
            tokbuf[block, rows], tokbuf[block, pl.ds(ROWS, MEM)], (((1,), (1,)), ((), ())),
            preferred_element_type=jnp.float32,
        )

    def left_rows(block):
        for c in (0, 1):
            to = 2 * block + c
            ref = tokbuf.at[block, pl.ds(ROWS, MEM), pl.ds(c * KB, KB)]

            @pl.when(to != p)
            def _():
                remote(ref, leftbuf.at[p], small_sent.at[0], small_got.at[0], (to, t)).start()

            @pl.when(to == p)
            def _():
                leftbuf[p] = ref[...]

    every = pl.ds(0, ROWS)

    def product(block):
        left_rows(block)
        base_rows(block, every)
        score_rows(block, every)

    def at_offset(ring, off):
        return ((z + off) % NZ) * 2 + (yh + ring) % 2

    def group_products(k):
        got(wbuf.at[pl.ds(0, NX)], cr.at[k])

        def body(i, _):
            product((group[k] * 2 + i) * 2 + yh)
            return 0

        lax.fori_loop(0, 2, body, 0)

    def ring_products(first, last):
        def body(i, _):
            odd = i % 2
            product(at_offset(1, (odd * ((i + 1) // 2) + (1 - odd) * (NZ - i // 2)) % NZ))
            return 0

        lax.fori_loop(first, last, body, 0)

    top, low = pl.ds(0, HALF), pl.ds(HALF, ROWS - HALF)

    loads[0].wait()
    loads[1].wait()
    zsend(0, 0)
    zsend(0, 1)
    tell(0)
    loads[2].wait()
    loads[3].wait()
    yown()
    to_relay(0, z)
    xsend(0)
    told(0)
    tell(1)

    zevent(0, 0)
    ywait(1)
    pl.when(middle)(functools.partial(ywait, 2))
    xwait(0)
    zevent(0, 1)
    told(1)
    from_relay(0, z)
    zevent(0, 2)
    zevent(0, 3)
    pl.when(middle)(functools.partial(ywait, 3))
    pl.when(edge)(functools.partial(ywait, 2))
    xwait(1)
    fwait(0)
    zevent(0, 4)
    zevent(0, 5)
    mate(0, z)
    zsend(1, 0)
    zsend(1, 1)
    xwait(2)
    zevent(0, 6)
    to_relay(1, z + 4)
    to_relay(2, z)
    pl.when(edge)(functools.partial(ywait, 3))
    fwait(1)
    zevent(1, 0)
    fwait(2)
    group_products(0)
    from_relay(1, z + 4)
    zevent(1, 1)
    from_relay(2, z)
    xwait(3)
    group_products(1)
    zevent(1, 2)
    group_products(2)
    fwait(3)
    zevent(1, 3)
    group_products(3)
    ring_products(0, 5)
    zevent(1, 4)
    before, after = at_offset(1, NZ - 3), at_offset(1, 3)
    base_rows(before, top)
    base_rows(after, low)
    score_rows(after, low)
    loads[4].wait()
    mate(1, z + 4)
    product(at_offset(1, 4))
    firsts = pl.ds(0, LAST), pl.ds(HALF, LAST)
    rests = pl.ds(LAST, HALF - LAST), pl.ds(HALF + LAST, ROWS - HALF - LAST)
    right_rows = wbuf[p, pl.ds(KB, MEM)].astype(jnp.float32)
    lane = lax.broadcasted_iota(jnp.int32, (LEN, MEM), 1)
    place = lax.broadcasted_iota(jnp.int32, (1, 128), 1)

    def finish(members, mine):
        for m in members:
            rows = pl.ds(m * LEN, LEN)
            s = jnp.sum(jnp.where(lane == m, sc[rows, :], 0.0), axis=1, keepdims=True)
            full = acc[rows, :] + (sigma_scale * s) * right_rows[m : m + 1, :] + tokbuf[t, rows].astype(jnp.float32)
            hid[rows, :] = full.astype(jnp.bfloat16)
            differ = full - tgt[rows, :].astype(jnp.float32)
            total = jnp.sum(jnp.sum(differ * differ, axis=0, keepdims=True), axis=1, keepdims=True)
            mine = mine + jnp.where(place == (p % 8) * MEM + m, total, 0.0)
        return mine

    mate(2, z)
    zevent(1, 5)
    for block, seen, scored in ((before, rests[1], (top, rests[1])), (after, rests[0], (rests[0],))):
        base_rows(block, seen)
        for rows in scored:
            score_rows(block, rows)
        left_rows(block)
    last_members = [m for m in range(MEM) if m * LEN % HALF < LAST]
    mine = finish([m for m in range(MEM) if m not in last_members], jnp.zeros((1, 128), jnp.float32))
    zevent(1, 6)
    for block, seen in ((before, firsts[1]), (after, firsts[0])):
        base_rows(block, seen)
        score_rows(block, seen)
    loss1[z * 2 + core] = finish(last_members, mine)

    ref = loss1.at[z * 2 + core]
    for dz in (4, 3, 5, 2, 6, 1, 7, 0):
        for dc in (1, 0):
            if dz or dc:
                dev = (pop_of(yl, x, (core + dc) % 2), ((z + dz) % NZ) * 2 + yh)
                remote(ref, ref, small_sent.at[1], small_got.at[1], dev).start()

    got(leftbuf.at[pl.ds(0, NPOP - 1)], small_got.at[0])
    left_t[...] = leftbuf[...].reshape(MEMBERS, KB).astype(jnp.float32).T

    got(loss1.at[pl.ds(0, 15)], small_got.at[1])
    row = loss1[0]
    for i in range(1, 16):
        row = row + loss1[i]
    loss2[y * NX + x] = row
    ref = loss2.at[y * NX + x]
    for dy in (4, 3, 5, 2, 6, 1, 7, 0):
        for dx in (2, 1, 3, 0):
            if dy or dx:
                remote(ref, ref, small_sent.at[2], small_got.at[2], at_yx((y + dy) % NY, (x + dx) % NX)).start()
    got(loss2.at[pl.ds(0, 31)], small_got.at[2])

    losses = []
    for q in range(NYL):
        row = loss2[q * NX]
        for i in range(1, NX):
            row = row + loss2[q * NX + i]
        for i in range(NX):
            row = row + loss2[(NYL + q) * NX + i]
        losses.append(row / (LEN * D))
    mean = jnp.sum(losses[0] + losses[1] + losses[2] + losses[3]) / MEMBERS
    squares = [row * row for row in losses]
    spread = jnp.sum(squares[0] + squares[1] + squares[2] + squares[3]) / MEMBERS - mean * mean
    root = jnp.sqrt(jnp.full((1, 128), spread + epsilon, jnp.float32))

    fitness = jnp.concatenate([-(row - mean) / root for row in losses], axis=1)
    weighted = left_t[...] * fitness
    b1 = weighted.astype(jnp.bfloat16)
    b2 = (weighted - b1.astype(jnp.float32)).astype(jnp.bfloat16)
    r = wbuf[:, pl.ds(KB, MEM)].reshape(MEMBERS, COLS)
    total = jnp.dot(jnp.concatenate([b2, b1], axis=0), r, preferred_element_type=jnp.float32)
    total = total[:KB] + total[KB:]
    upd[...] = total * (1.0 / (MEMBERS * sigma_scale))

    left_device(tokbuf, z_sent.at[0])
    left_device(tokbuf.at[pl.ds(0, 2), pl.ds(0, HALF + EXTRA + MEM)], z_sent.at[1])
    left_device(wbuf.at[pl.ds(0, 28)], w_sent)
    @pl.when(middle)
    def _():
        left_device(wbuf.at[pl.ds(0, 5)], y_sent)

    @pl.when(edge)
    def _():
        left_device(wbuf.at[0], y_sent)

    left_device(leftbuf.at[pl.ds(0, NPOP - 1)], small_sent.at[0])
    left_device(loss1.at[pl.ds(0, 15)], small_sent.at[1])
    left_device(loss2.at[pl.ds(0, 31)], small_sent.at[2])


def write_out(hid, upd, hid_hbm, upd_hbm, sem):
    copies = [pltpu.make_async_copy(hid, hid_hbm, sem.at[0]), pltpu.make_async_copy(upd, upd_hbm, sem.at[1])]
    for c in copies:
        c.start()
    for c in copies:
        c.wait()


def per_device(tokens, weight, left, right, target):
    dma = pltpu.SemaphoreType.DMA
    bf, f32 = jnp.bfloat16, jnp.float32
    hidden, update = pl.pallas_call(
        kernel,
        out_shape=(pltpu.VMEM((ROWS, COLS), bf), pltpu.VMEM((KB, COLS), f32)),
        in_specs=[pl.BlockSpec(memory_space=pl.ANY)] * 5,
        out_specs=(pl.BlockSpec(memory_space=pltpu.VMEM), pl.BlockSpec(memory_space=pltpu.VMEM)),
        scratch_shapes=[
            pltpu.VMEM((NTP, TB, COLS), bf),
            pltpu.VMEM((NPOP, WB, COLS), bf),
            pltpu.VMEM((3, HALF, COLS), bf),
            pltpu.VMEM((3, TB - HALF, COLS), bf),
            pltpu.VMEM((ROWS, COLS), f32),
            pltpu.VMEM((ROWS, MEM), f32),
            pltpu.VMEM((ROWS, COLS), bf),
            pltpu.VMEM((NPOP, MEM, KB), bf),
            pltpu.VMEM((KB, MEMBERS), f32),
            pltpu.VMEM((16, 1, 128), f32),
            pltpu.VMEM((32, 1, 128), f32),
            dma((5,)),
            dma((2,)), dma((2, 2, 7)), dma((3,)), dma((3,)),
            dma(()), dma(()), dma((NYL,)), dma((4,)), dma((4,)), dma((4,)),
            dma((3,)), dma((3,)),
            pltpu.SemaphoreType.REGULAR((2,)),
        ],
        compiler_params=pltpu.CompilerParams(
            collective_id=0, has_side_effects=True, vmem_limit_bytes=56 * 1024 * 1024
        ),
    )(tokens, weight, left, right, target)
    return pl.pallas_call(
        write_out,
        out_shape=(jax.ShapeDtypeStruct((ROWS, COLS), bf), jax.ShapeDtypeStruct((KB, COLS), f32)),
        in_specs=[pl.BlockSpec(memory_space=pl.ANY)] * 2,
        out_specs=(pl.BlockSpec(memory_space=pl.ANY), pl.BlockSpec(memory_space=pl.ANY)),
        scratch_shapes=[dma((2,))],
        compiler_params=pltpu.CompilerParams(vmem_limit_bytes=1024 * 1024),
    )(hidden, update)


def solution(mesh):
    return jax.shard_map(
        per_device,
        mesh=mesh,
        in_specs=(P("pop", "tp"), P("pop", "tp"), P("pop", "tp"), P("pop", "tp"), P("pop", "tp")),
        out_specs=(P("pop", "tp"), P("pop", "tp")),
        check_vma=False,
    )
```

```python
import functools

import jax
import jax.numpy as jnp
from jax import lax
from jax.experimental import pallas as pl
from jax.experimental.pallas import tpu as pltpu
from jax.sharding import PartitionSpec as P

D = 8192
LEN = 32
MEMBERS = 512

sigma_scale = 0.5
epsilon = 1e-06

MESH = pl.DeviceIdType.MESH
NX, NY, NYL, NZ = 4, 8, 4, 8
NPOP, NTP = 32, 16
ROWS = 512
COLS = 512
KB = 256
MEM = 16
TB = ROWS + MEM
WB = KB + MEM
LAST = 96
EXTRA = 32
HALF = 256
WHALF = 128


def kernel(
    tok_hbm, w_hbm, left_hbm, right_hbm, tgt_hbm, hid, upd,
    tokbuf, wbuf, relay_a, relay_b, acc, sc, tgt, leftbuf, left_t, loss1, loss2,
    loc, z_sent, zr, rr, mr, y_sent, w_sent, yr, xr, fr, cr, small_sent, small_got,
    entered,
):
    p = lax.axis_index("pop")
    t = lax.axis_index("tp")
    core = p % 2
    x = (p // 2) % NX
    yl = p // (2 * NX)
    z = t // 2
    yh = t % 2
    y = yh * NYL + yl

    def pop_of(yl_, x_, c_):
        return (yl_ * NX + x_) * 2 + c_

    def at_yx(y_, x_):
        return (pop_of(y_ % NYL, x_, core), z * 2 + y_ // NYL)

    def at_y(y_):
        return at_yx(y_ % NY, x)

    def at_x(x_):
        return (pop_of(yl, x_ % NX, core), t)

    def at_z(z_):
        return (p, (z_ % NZ) * 2 + yh)

    other_core = (pop_of(yl, x, 1 - core), t)

    middle = (yl == 1) | (yl == 2)
    edge = jnp.logical_not(middle)

    barrier = pltpu.get_barrier_semaphore()
    near = [at_z(z + 1), at_z(z + NZ - 1), at_y(y + 1), at_y(y + NY - 1), at_x(x + 1), at_x(x + NX - 1), other_core]
    for d in near:
        pl.semaphore_signal(barrier, inc=1, device_id=d, device_id_type=MESH)
    loads = [
        pltpu.make_async_copy(tok_hbm, tokbuf.at[t, pl.ds(0, ROWS)], loc.at[0]),
        pltpu.make_async_copy(left_hbm, tokbuf.at[t, pl.ds(ROWS, MEM)], loc.at[1]),
        pltpu.make_async_copy(w_hbm, wbuf.at[p, pl.ds(0, KB)], loc.at[2]),
        pltpu.make_async_copy(right_hbm, wbuf.at[p, pl.ds(KB, MEM)], loc.at[3]),
        pltpu.make_async_copy(tgt_hbm, tgt, loc.at[4]),
    ]
    for c in loads:
        c.start()

    acc[...] = jnp.zeros_like(acc)
    sc[...] = jnp.zeros_like(sc)
    pl.semaphore_wait(barrier, len(near))

    def remote(src, dst, s, r, dev):
        return pltpu.make_async_remote_copy(
            src_ref=src, dst_ref=dst, send_sem=s, recv_sem=r, device_id=dev, device_id_type=MESH
        )

    def got(ref, sem):
        remote(ref, ref, z_sent.at[0], sem, other_core).wait_recv()

    def left_device(ref, sem):
        remote(ref, ref, sem, mr.at[0], other_core).wait_send()

    def chunk(block, c):
        return tokbuf.at[block, pl.ds(0, HALF)] if c == 0 else tokbuf.at[block, pl.ds(HALF, TB - HALF)]

    def ring_chunk(ring, way, j, dist):
        c = j % 2 if way == 0 else 1 - j % 2
        src_z = z + NZ - dist if way == 0 else z + dist
        block = (src_z % NZ) * 2 + (yh if ring == 0 else 1 - yh)
        if ring == 1 and j >= 5:
            c = 1 - way
            start, rows = (0, LAST) if j == 6 else (LAST, HALF - EXTRA - LAST)
            return tokbuf.at[block, pl.ds(c * HALF + start, rows)]
        return chunk(block, c)

    def zsend(ring, j):
        for way in (0, 1):
            zsend_way(ring, way, j)

    def zsend_way(ring, way, j):
        ref = ring_chunk(ring, way, j, min(j // 2, 2 if ring == 1 else 3))
        dev = at_z(z + 1) if way == 0 else at_z(z + NZ - 1)
        small = ring == 1 and j >= 5
        remote(ref, ref, z_sent.at[1 if small else 0], zr.at[way, ring, j], dev).start()

    def zevent(ring, j):
        for way in (0, 1):
            got(ring_chunk(ring, way, j, min(j // 2, 2 if ring == 1 else 3) + 1), zr.at[way, ring, j])
            if j + 2 < 7 - ring:
                zsend_way(ring, way, j + 2)
            if ring == 1 and j == 3:
                zsend_way(1, way, 6)

    def pieces(n, own_yh, src_z):
        if n < 2:
            block = (src_z % NZ) * 2 + own_yh
            return chunk(block, 0), chunk(block, 1)
        after, before = ((z + 3) % NZ) * 2 + own_yh, ((z + NZ - 3) % NZ) * 2 + own_yh
        return tokbuf.at[after, pl.ds(HALF - EXTRA, EXTRA)], tokbuf.at[before, pl.ds(ROWS - EXTRA, EXTRA + MEM)]

    def relay(n):
        if n < 2:
            return relay_a.at[n], relay_b.at[n]
        return relay_a.at[n, pl.ds(0, EXTRA)], relay_b.at[n, pl.ds(0, EXTRA + MEM)]

    def to_relay(n, src_z):
        for way, ref, buf, dev in zip((0, 1), pieces(n, yh, src_z), relay(n), (at_y(y + 1), at_y(y + NY - 1))):
            remote(ref, buf, z_sent.at[n // 2], rr.at[n], dev).start()

    def from_relay(n, src_z):
        got(tokbuf.at[0] if n < 2 else tokbuf.at[0, pl.ds(0, 2 * EXTRA + MEM)], rr.at[n])
        for way, buf, step in zip((0, 1), relay(n), (3, NY - 3)):
            y_to = (y + step) % NY
            dst = pieces(n, (y_to + NYL) % NY // NYL, src_z)[way]
            remote(buf, dst, z_sent.at[n // 2], mr.at[n], at_y(y_to)).start()

    def mate(n, src_z):
        if n < 2:
            got(tokbuf.at[(src_z % NZ) * 2 + (1 - yh)], mr.at[n])
        else:
            got(tokbuf.at[0, pl.ds(0, 2 * EXTRA + MEM)], mr.at[n])

    def tell(n):
        for dev in (at_y(y + 1), at_y(y + NY - 1)):
            pl.semaphore_signal(entered.at[n], inc=1, device_id=dev, device_id_type=MESH)

    def told(n):
        pl.semaphore_wait(entered.at[n], 2)

    near_y = yl - 1 + 2 * ((3 - yl) // 3)
    far_y = 3 * ((3 - yl) // 2)
    group = (yl, near_y, 6 - yl - near_y - far_y, far_y)

    def wblock(k, dx):
        return wbuf.at[pop_of(group[k], (x + dx + NX) % NX, core)]

    def csend(k, dx):
        ref = wblock(k, dx)
        remote(ref, ref, w_sent, cr.at[k], other_core).start()

    def xsend(k):
        ref = wblock(k, 0)
        remote(ref, ref, w_sent, xr.at[k], at_x(x + 1)).start()
        remote(ref, ref, w_sent, xr.at[k], at_x(x + NX - 1)).start()
        csend(k, 0)

    def ysend(k, up, down):
        ref = wblock(k, 0)

        @pl.when(up)
        def _():
            remote(ref, ref, y_sent, yr.at[group[k]], (pop_of((yl + 1) % NYL, x, core), t)).start()

        @pl.when(down)
        def _():
            remote(ref, ref, y_sent, yr.at[group[k]], (pop_of((yl + NYL - 1) % NYL, x, core), t)).start()

    def yown():
        ysend(0, yl < NYL - 1, yl > 0)

    def ywait(k):
        src = group[k]
        got(wblock(k, 0), yr.at[src])
        ysend(k, (src < yl) & (yl < NYL - 1), (src > yl) & (yl > 0))
        xsend(k)

    lo, hi = pl.ds(0, WHALF), pl.ds(WHALF, WB - WHALF)

    def xwait(k):
        got(wbuf.at[pl.ds(0, 2)], xr.at[k])
        for dx, part, dev in ((-1, lo, at_x(x + 1)), (1, hi, at_x(x + NX - 1))):
            ref = wblock(k, dx).at[part]
            remote(ref, ref, w_sent, fr.at[k], dev).start()
            csend(k, dx)

    def fwait(k):
        got(wblock(k, 2), fr.at[k])
        csend(k, 2)

    def base_rows(block, rows):
        a = tokbuf[block, rows]
        acc[rows, :] += jnp.dot(
            a[:, :KB], wbuf[2 * block, pl.ds(0, KB)], preferred_element_type=jnp.float32
        ) + jnp.dot(a[:, KB:], wbuf[2 * block + 1, pl.ds(0, KB)], preferred_element_type=jnp.float32)

    def score_rows(block, rows):
        sc[rows, :] += lax.dot_general(
            tokbuf[block, rows], tokbuf[block, pl.ds(ROWS, MEM)], (((1,), (1,)), ((), ())),
            preferred_element_type=jnp.float32,
        )

    def left_rows(block):
        for c in (0, 1):
            to = 2 * block + c
            ref = tokbuf.at[block, pl.ds(ROWS, MEM), pl.ds(c * KB, KB)]

            @pl.when(to != p)
            def _():
                remote(ref, leftbuf.at[p], small_sent.at[0], small_got.at[0], (to, t)).start()

            @pl.when(to == p)
            def _():
                leftbuf[p] = ref[...]

    every = pl.ds(0, ROWS)

    def product(block):
        left_rows(block)
        base_rows(block, every)
        score_rows(block, every)

    def at_offset(ring, off):
        return ((z + off) % NZ) * 2 + (yh + ring) % 2

    def group_products(k):
        got(wbuf.at[pl.ds(0, NX)], cr.at[k])

        def body(i, _):
            product((group[k] * 2 + i) * 2 + yh)
            return 0

        lax.fori_loop(0, 2, body, 0)

    def ring_products(first, last):
        def body(i, _):
            odd = i % 2
            product(at_offset(1, (odd * ((i + 1) // 2) + (1 - odd) * (NZ - i // 2)) % NZ))
            return 0

        lax.fori_loop(first, last, body, 0)

    top, low = pl.ds(0, HALF), pl.ds(HALF, ROWS - HALF)

    loads[0].wait()
    loads[1].wait()
    zsend(0, 0)
    zsend(0, 1)
    tell(0)
    loads[2].wait()
    loads[3].wait()
    yown()
    to_relay(0, z)
    xsend(0)
    told(0)
    tell(1)

    zevent(0, 0)
    ywait(1)
    pl.when(middle)(functools.partial(ywait, 2))
    xwait(0)
    zevent(0, 1)
    told(1)
    from_relay(0, z)
    zevent(0, 2)
    zevent(0, 3)
    pl.when(middle)(functools.partial(ywait, 3))
    pl.when(edge)(functools.partial(ywait, 2))
    xwait(1)
    fwait(0)
    zevent(0, 4)
    zevent(0, 5)
    mate(0, z)
    zsend(1, 0)
    zsend(1, 1)
    xwait(2)
    zevent(0, 6)
    to_relay(1, z + 4)
    to_relay(2, z)
    pl.when(edge)(functools.partial(ywait, 3))
    fwait(1)
    zevent(1, 0)
    fwait(2)
    group_products(0)
    from_relay(1, z + 4)
    zevent(1, 1)
    from_relay(2, z)
    xwait(3)
    group_products(1)
    zevent(1, 2)
    group_products(2)
    fwait(3)
    zevent(1, 3)
    group_products(3)
    ring_products(0, 5)
    zevent(1, 4)
    before, after = at_offset(1, NZ - 3), at_offset(1, 3)
    base_rows(before, top)
    base_rows(after, low)
    score_rows(after, low)
    loads[4].wait()
    mate(1, z + 4)
    product(at_offset(1, 4))
    firsts = pl.ds(0, LAST), pl.ds(HALF, LAST)
    rests = pl.ds(LAST, HALF - LAST), pl.ds(HALF + LAST, ROWS - HALF - LAST)
    right_rows = wbuf[p, pl.ds(KB, MEM)].astype(jnp.float32)
    lane = lax.broadcasted_iota(jnp.int32, (LEN, MEM), 1)
    place = lax.broadcasted_iota(jnp.int32, (1, 128), 1)

    def finish(members, mine):
        for m in members:
            rows = pl.ds(m * LEN, LEN)
            s = jnp.sum(jnp.where(lane == m, sc[rows, :], 0.0), axis=1, keepdims=True)
            full = acc[rows, :] + (sigma_scale * s) * right_rows[m : m + 1, :] + tokbuf[t, rows].astype(jnp.float32)
            hid[rows, :] = full.astype(jnp.bfloat16)
            differ = full - tgt[rows, :].astype(jnp.float32)
            total = jnp.sum(jnp.sum(differ * differ, axis=0, keepdims=True), axis=1, keepdims=True)
            mine = mine + jnp.where(place == (p % 8) * MEM + m, total, 0.0)
        return mine

    mate(2, z)
    zevent(1, 5)
    for block, seen, scored in ((before, rests[1], (top, rests[1])), (after, rests[0], (rests[0],))):
        base_rows(block, seen)
        for rows in scored:
            score_rows(block, rows)
        left_rows(block)
    last_members = [m for m in range(MEM) if m * LEN % HALF < LAST]
    mine = finish([m for m in range(MEM) if m not in last_members], jnp.zeros((1, 128), jnp.float32))
    zevent(1, 6)
    for block, seen in ((before, firsts[1]), (after, firsts[0])):
        base_rows(block, seen)
        score_rows(block, seen)
    loss1[z * 2 + core] = finish(last_members, mine)

    ref = loss1.at[z * 2 + core]
    for dz in (4, 3, 5, 2, 6, 1, 7, 0):
        for dc in (1, 0):
            if dz or dc:
                dev = (pop_of(yl, x, (core + dc) % 2), ((z + dz) % NZ) * 2 + yh)
                remote(ref, ref, small_sent.at[1], small_got.at[1], dev).start()

    got(leftbuf.at[pl.ds(0, NPOP - 1)], small_got.at[0])
    left_t[...] = leftbuf[...].reshape(MEMBERS, KB).astype(jnp.float32).T

    got(loss1.at[pl.ds(0, 15)], small_got.at[1])
    row = loss1[0]
    for i in range(1, 16):
        row = row + loss1[i]
    loss2[y * NX + x] = row
    ref = loss2.at[y * NX + x]
    for dy in (4, 3, 5, 2, 6, 1, 7, 0):
        for dx in (2, 1, 3, 0):
            if dy or dx:
                remote(ref, ref, small_sent.at[2], small_got.at[2], at_yx((y + dy) % NY, (x + dx) % NX)).start()
    got(loss2.at[pl.ds(0, 31)], small_got.at[2])

    losses = []
    for q in range(NYL):
        row = loss2[q * NX]
        for i in range(1, NX):
            row = row + loss2[q * NX + i]
        for i in range(NX):
            row = row + loss2[(NYL + q) * NX + i]
        losses.append(row / (LEN * D))
    mean = jnp.sum(losses[0] + losses[1] + losses[2] + losses[3]) / MEMBERS
    squares = [row * row for row in losses]
    spread = jnp.sum(squares[0] + squares[1] + squares[2] + squares[3]) / MEMBERS - mean * mean
    root = jnp.sqrt(jnp.full((1, 128), spread + epsilon, jnp.float32))

    fitness = jnp.concatenate([-(row - mean) / root for row in losses], axis=1)
    weighted = left_t[...] * fitness
    b1 = weighted.astype(jnp.bfloat16)
    b2 = (weighted - b1.astype(jnp.float32)).astype(jnp.bfloat16)
    r = wbuf[:, pl.ds(KB, MEM)].reshape(MEMBERS, COLS)
    total = jnp.dot(jnp.concatenate([b2, b1], axis=0), r, preferred_element_type=jnp.float32)
    total = total[:KB] + total[KB:]
    upd[...] = total * (1.0 / (MEMBERS * sigma_scale))

    left_device(tokbuf, z_sent.at[0])
    left_device(tokbuf.at[pl.ds(0, 2), pl.ds(0, HALF + EXTRA + MEM)], z_sent.at[1])
    left_device(wbuf.at[pl.ds(0, 28)], w_sent)
    @pl.when(middle)
    def _():
        left_device(wbuf.at[pl.ds(0, 5)], y_sent)

    @pl.when(edge)
    def _():
        left_device(wbuf.at[0], y_sent)

    left_device(leftbuf.at[pl.ds(0, NPOP - 1)], small_sent.at[0])
    left_device(loss1.at[pl.ds(0, 15)], small_sent.at[1])
    left_device(loss2.at[pl.ds(0, 31)], small_sent.at[2])


def write_out(hid, upd, hid_hbm, upd_hbm, sem):
    copies = [pltpu.make_async_copy(hid, hid_hbm, sem.at[0]), pltpu.make_async_copy(upd, upd_hbm, sem.at[1])]
    for c in copies:
        c.start()
    for c in copies:
        c.wait()


def per_device(tokens, weight, left, right, target):
    dma = pltpu.SemaphoreType.DMA
    bf, f32 = jnp.bfloat16, jnp.float32
    hidden, update = pl.pallas_call(
        kernel,
        out_shape=(pltpu.VMEM((ROWS, COLS), bf), pltpu.VMEM((KB, COLS), f32)),
        in_specs=[pl.BlockSpec(memory_space=pl.ANY)] * 5,
        out_specs=(pl.BlockSpec(memory_space=pltpu.VMEM), pl.BlockSpec(memory_space=pltpu.VMEM)),
        scratch_shapes=[
            pltpu.VMEM((NTP, TB, COLS), bf),
            pltpu.VMEM((NPOP, WB, COLS), bf),
            pltpu.VMEM((3, HALF, COLS), bf),
            pltpu.VMEM((3, TB - HALF, COLS), bf),
            pltpu.VMEM((ROWS, COLS), f32),
            pltpu.VMEM((ROWS, MEM), f32),
            pltpu.VMEM((ROWS, COLS), bf),
            pltpu.VMEM((NPOP, MEM, KB), bf),
            pltpu.VMEM((KB, MEMBERS), f32),
            pltpu.VMEM((16, 1, 128), f32),
            pltpu.VMEM((32, 1, 128), f32),
            dma((5,)),
            dma((2,)), dma((2, 2, 7)), dma((3,)), dma((3,)),
            dma(()), dma(()), dma((NYL,)), dma((4,)), dma((4,)), dma((4,)),
            dma((3,)), dma((3,)),
            pltpu.SemaphoreType.REGULAR((2,)),
        ],
        compiler_params=pltpu.CompilerParams(
            collective_id=0, has_side_effects=True, vmem_limit_bytes=56 * 1024 * 1024
        ),
    )(tokens, weight, left, right, target)
    return pl.pallas_call(
        write_out,
        out_shape=(jax.ShapeDtypeStruct((ROWS, COLS), bf), jax.ShapeDtypeStruct((KB, COLS), f32)),
        in_specs=[pl.BlockSpec(memory_space=pl.ANY)] * 2,
        out_specs=(pl.BlockSpec(memory_space=pl.ANY), pl.BlockSpec(memory_space=pl.ANY)),
        scratch_shapes=[dma((2,))],
        compiler_params=pltpu.CompilerParams(vmem_limit_bytes=1024 * 1024),
    )(hidden, update)


def solution(mesh):
    return jax.shard_map(
        per_device,
        mesh=mesh,
        in_specs=(P("pop", "tp"), P("pop", "tp"), P("pop", "tp"), P("pop", "tp"), P("pop", "tp")),
        out_specs=(P("pop", "tp"), P("pop", "tp")),
        check_vma=False,
    )
```

```python
import functools

import jax
import jax.numpy as jnp
from jax import lax
from jax.experimental import pallas as pl
from jax.experimental.pallas import tpu as pltpu
from jax.sharding import PartitionSpec as P

D = 8192
LEN = 32
MEMBERS = 512

sigma_scale = 0.5
epsilon = 1e-06

MESH = pl.DeviceIdType.MESH
NX, NY, NYL, NZ = 4, 8, 4, 8
NPOP, NTP = 32, 16
ROWS = 512
COLS = 512
KB = 256
MEM = 16
TB = ROWS + MEM
WB = KB + MEM
LAST = 96
EXTRA = 32
HALF = 256
WHALF = 128


def kernel(
    tok_hbm, w_hbm, left_hbm, right_hbm, tgt_hbm, hid, upd,
    tokbuf, wbuf, relay_a, relay_b, acc, sc, tgt, leftbuf, left_t, loss1, loss2,
    loc, z_sent, zr, rr, mr, y_sent, w_sent, yr, xr, fr, cr, small_sent, small_got,
    entered,
):
    p = lax.axis_index("pop")
    t = lax.axis_index("tp")
    core = p % 2
    x = (p // 2) % NX
    yl = p // (2 * NX)
    z = t // 2
    yh = t % 2
    y = yh * NYL + yl

    def pop_of(yl_, x_, c_):
        return (yl_ * NX + x_) * 2 + c_

    def at_yx(y_, x_):
        return (pop_of(y_ % NYL, x_, core), z * 2 + y_ // NYL)

    def at_y(y_):
        return at_yx(y_ % NY, x)

    def at_x(x_):
        return (pop_of(yl, x_ % NX, core), t)

    def at_z(z_):
        return (p, (z_ % NZ) * 2 + yh)

    other_core = (pop_of(yl, x, 1 - core), t)

    middle = (yl == 1) | (yl == 2)
    edge = jnp.logical_not(middle)

    barrier = pltpu.get_barrier_semaphore()
    near = [at_z(z + 1), at_z(z + NZ - 1), at_y(y + 1), at_y(y + NY - 1), at_x(x + 1), at_x(x + NX - 1), other_core]
    for d in near:
        pl.semaphore_signal(barrier, inc=1, device_id=d, device_id_type=MESH)
    loads = [
        pltpu.make_async_copy(tok_hbm, tokbuf.at[t, pl.ds(0, ROWS)], loc.at[0]),
        pltpu.make_async_copy(left_hbm, tokbuf.at[t, pl.ds(ROWS, MEM)], loc.at[1]),
        pltpu.make_async_copy(w_hbm, wbuf.at[p, pl.ds(0, KB)], loc.at[2]),
        pltpu.make_async_copy(right_hbm, wbuf.at[p, pl.ds(KB, MEM)], loc.at[3]),
        pltpu.make_async_copy(tgt_hbm, tgt, loc.at[4]),
    ]
    for c in loads:
        c.start()

    acc[...] = jnp.zeros_like(acc)
    sc[...] = jnp.zeros_like(sc)
    pl.semaphore_wait(barrier, len(near))

    def remote(src, dst, s, r, dev):
        return pltpu.make_async_remote_copy(
            src_ref=src, dst_ref=dst, send_sem=s, recv_sem=r, device_id=dev, device_id_type=MESH
        )

    def got(ref, sem):
        remote(ref, ref, z_sent.at[0], sem, other_core).wait_recv()

    def left_device(ref, sem):
        remote(ref, ref, sem, mr.at[0], other_core).wait_send()

    def chunk(block, c):
        return tokbuf.at[block, pl.ds(0, HALF)] if c == 0 else tokbuf.at[block, pl.ds(HALF, TB - HALF)]

    def ring_chunk(ring, way, j, dist):
        c = j % 2 if way == 0 else 1 - j % 2
        src_z = z + NZ - dist if way == 0 else z + dist
        block = (src_z % NZ) * 2 + (yh if ring == 0 else 1 - yh)
        if ring == 1 and j >= 5:
            c = 1 - way
            start, rows = (0, LAST) if j == 6 else (LAST, HALF - EXTRA - LAST)
            return tokbuf.at[block, pl.ds(c * HALF + start, rows)]
        return chunk(block, c)

    def zsend(ring, j):
        for way in (0, 1):
            zsend_way(ring, way, j)

    def zsend_way(ring, way, j):
        ref = ring_chunk(ring, way, j, min(j // 2, 2 if ring == 1 else 3))
        dev = at_z(z + 1) if way == 0 else at_z(z + NZ - 1)
        small = ring == 1 and j >= 5
        remote(ref, ref, z_sent.at[1 if small else 0], zr.at[way, ring, j], dev).start()

    def zevent(ring, j):
        for way in (0, 1):
            got(ring_chunk(ring, way, j, min(j // 2, 2 if ring == 1 else 3) + 1), zr.at[way, ring, j])
            if j + 2 < 7 - ring:
                zsend_way(ring, way, j + 2)
            if ring == 1 and j == 3:
                zsend_way(1, way, 6)

    def pieces(n, own_yh, src_z):
        if n < 2:
            block = (src_z % NZ) * 2 + own_yh
            return chunk(block, 0), chunk(block, 1)
        after, before = ((z + 3) % NZ) * 2 + own_yh, ((z + NZ - 3) % NZ) * 2 + own_yh
        return tokbuf.at[after, pl.ds(HALF - EXTRA, EXTRA)], tokbuf.at[before, pl.ds(ROWS - EXTRA, EXTRA + MEM)]

    def relay(n):
        if n < 2:
            return relay_a.at[n], relay_b.at[n]
        return relay_a.at[n, pl.ds(0, EXTRA)], relay_b.at[n, pl.ds(0, EXTRA + MEM)]

    def to_relay(n, src_z):
        for way, ref, buf, dev in zip((0, 1), pieces(n, yh, src_z), relay(n), (at_y(y + 1), at_y(y + NY - 1))):
            remote(ref, buf, z_sent.at[n // 2], rr.at[n], dev).start()

    def from_relay(n, src_z):
        got(tokbuf.at[0] if n < 2 else tokbuf.at[0, pl.ds(0, 2 * EXTRA + MEM)], rr.at[n])
        for way, buf, step in zip((0, 1), relay(n), (3, NY - 3)):
            y_to = (y + step) % NY
            dst = pieces(n, (y_to + NYL) % NY // NYL, src_z)[way]
            remote(buf, dst, z_sent.at[n // 2], mr.at[n], at_y(y_to)).start()

    def mate(n, src_z):
        if n < 2:
            got(tokbuf.at[(src_z % NZ) * 2 + (1 - yh)], mr.at[n])
        else:
            got(tokbuf.at[0, pl.ds(0, 2 * EXTRA + MEM)], mr.at[n])

    def tell(n):
        for dev in (at_y(y + 1), at_y(y + NY - 1)):
            pl.semaphore_signal(entered.at[n], inc=1, device_id=dev, device_id_type=MESH)

    def told(n):
        pl.semaphore_wait(entered.at[n], 2)

    near_y = yl - 1 + 2 * ((3 - yl) // 3)
    far_y = 3 * ((3 - yl) // 2)
    group = (yl, near_y, 6 - yl - near_y - far_y, far_y)

    def wblock(k, dx):
        return wbuf.at[pop_of(group[k], (x + dx + NX) % NX, core)]

    def csend(k, dx):
        ref = wblock(k, dx)
        remote(ref, ref, w_sent, cr.at[k], other_core).start()

    def xsend(k):
        ref = wblock(k, 0)
        remote(ref, ref, w_sent, xr.at[k], at_x(x + 1)).start()
        remote(ref, ref, w_sent, xr.at[k], at_x(x + NX - 1)).start()
        csend(k, 0)

    def ysend(k, up, down):
        ref = wblock(k, 0)

        @pl.when(up)
        def _():
            remote(ref, ref, y_sent, yr.at[group[k]], (pop_of((yl + 1) % NYL, x, core), t)).start()

        @pl.when(down)
        def _():
            remote(ref, ref, y_sent, yr.at[group[k]], (pop_of((yl + NYL - 1) % NYL, x, core), t)).start()

    def yown():
        ysend(0, yl < NYL - 1, yl > 0)

    def ywait(k):
        src = group[k]
        got(wblock(k, 0), yr.at[src])
        ysend(k, (src < yl) & (yl < NYL - 1), (src > yl) & (yl > 0))
        xsend(k)

    lo, hi = pl.ds(0, WHALF), pl.ds(WHALF, WB - WHALF)

    def xwait(k):
        got(wbuf.at[pl.ds(0, 2)], xr.at[k])
        for dx, part, dev in ((-1, lo, at_x(x + 1)), (1, hi, at_x(x + NX - 1))):
            ref = wblock(k, dx).at[part]
            remote(ref, ref, w_sent, fr.at[k], dev).start()
            csend(k, dx)

    def fwait(k):
        got(wblock(k, 2), fr.at[k])
        csend(k, 2)

    def base_rows(block, rows):
        a = tokbuf[block, rows]
        acc[rows, :] += jnp.dot(
            a[:, :KB], wbuf[2 * block, pl.ds(0, KB)], preferred_element_type=jnp.float32
        ) + jnp.dot(a[:, KB:], wbuf[2 * block + 1, pl.ds(0, KB)], preferred_element_type=jnp.float32)

    def score_rows(block, rows):
        sc[rows, :] += lax.dot_general(
            tokbuf[block, rows], tokbuf[block, pl.ds(ROWS, MEM)], (((1,), (1,)), ((), ())),
            preferred_element_type=jnp.float32,
        )

    def left_rows(block):
        for c in (0, 1):
            to = 2 * block + c
            ref = tokbuf.at[block, pl.ds(ROWS, MEM), pl.ds(c * KB, KB)]

            @pl.when(to != p)
            def _():
                remote(ref, leftbuf.at[p], small_sent.at[0], small_got.at[0], (to, t)).start()

            @pl.when(to == p)
            def _():
                leftbuf[p] = ref[...]

    every = pl.ds(0, ROWS)

    def product(block):
        left_rows(block)
        base_rows(block, every)
        score_rows(block, every)

    def at_offset(ring, off):
        return ((z + off) % NZ) * 2 + (yh + ring) % 2

    def group_products(k):
        got(wbuf.at[pl.ds(0, NX)], cr.at[k])

        def body(i, _):
            product((group[k] * 2 + i) * 2 + yh)
            return 0

        lax.fori_loop(0, 2, body, 0)

    def ring_products(first, last):
        def body(i, _):
            odd = i % 2
            product(at_offset(1, (odd * ((i + 1) // 2) + (1 - odd) * (NZ - i // 2)) % NZ))
            return 0

        lax.fori_loop(first, last, body, 0)

    top, low = pl.ds(0, HALF), pl.ds(HALF, ROWS - HALF)

    loads[0].wait()
    loads[1].wait()
    zsend(0, 0)
    zsend(0, 1)
    tell(0)
    loads[2].wait()
    loads[3].wait()
    yown()
    to_relay(0, z)
    xsend(0)
    told(0)
    tell(1)

    zevent(0, 0)
    ywait(1)
    pl.when(middle)(functools.partial(ywait, 2))
    xwait(0)
    zevent(0, 1)
    told(1)
    from_relay(0, z)
    zevent(0, 2)
    zevent(0, 3)
    pl.when(middle)(functools.partial(ywait, 3))
    pl.when(edge)(functools.partial(ywait, 2))
    xwait(1)
    fwait(0)
    zevent(0, 4)
    zevent(0, 5)
    mate(0, z)
    zsend(1, 0)
    zsend(1, 1)
    xwait(2)
    zevent(0, 6)
    to_relay(1, z + 4)
    to_relay(2, z)
    pl.when(edge)(functools.partial(ywait, 3))
    fwait(1)
    zevent(1, 0)
    fwait(2)
    group_products(0)
    from_relay(1, z + 4)
    zevent(1, 1)
    from_relay(2, z)
    xwait(3)
    group_products(1)
    zevent(1, 2)
    group_products(2)
    fwait(3)
    zevent(1, 3)
    group_products(3)
    ring_products(0, 5)
    zevent(1, 4)
    before, after = at_offset(1, NZ - 3), at_offset(1, 3)
    base_rows(before, top)
    base_rows(after, low)
    score_rows(after, low)
    loads[4].wait()
    mate(1, z + 4)
    product(at_offset(1, 4))
    firsts = pl.ds(0, LAST), pl.ds(HALF, LAST)
    rests = pl.ds(LAST, HALF - LAST), pl.ds(HALF + LAST, ROWS - HALF - LAST)
    right_rows = wbuf[p, pl.ds(KB, MEM)].astype(jnp.float32)
    lane = lax.broadcasted_iota(jnp.int32, (LEN, MEM), 1)
    place = lax.broadcasted_iota(jnp.int32, (1, 128), 1)

    def finish(members, mine):
        for m in members:
            rows = pl.ds(m * LEN, LEN)
            s = jnp.sum(jnp.where(lane == m, sc[rows, :], 0.0), axis=1, keepdims=True)
            full = acc[rows, :] + (sigma_scale * s) * right_rows[m : m + 1, :] + tokbuf[t, rows].astype(jnp.float32)
            hid[rows, :] = full.astype(jnp.bfloat16)
            differ = full - tgt[rows, :].astype(jnp.float32)
            total = jnp.sum(jnp.sum(differ * differ, axis=0, keepdims=True), axis=1, keepdims=True)
            mine = mine + jnp.where(place == (p % 8) * MEM + m, total, 0.0)
        return mine

    mate(2, z)
    zevent(1, 5)
    for block, seen, scored in ((before, rests[1], (top, rests[1])), (after, rests[0], (rests[0],))):
        base_rows(block, seen)
        for rows in scored:
            score_rows(block, rows)
        left_rows(block)
    last_members = [m for m in range(MEM) if m * LEN % HALF < LAST]
    mine = finish([m for m in range(MEM) if m not in last_members], jnp.zeros((1, 128), jnp.float32))
    zevent(1, 6)
    for block, seen in ((before, firsts[1]), (after, firsts[0])):
        base_rows(block, seen)
        score_rows(block, seen)
    loss1[z * 2 + core] = finish(last_members, mine)

    ref = loss1.at[z * 2 + core]
    for dz in (4, 3, 5, 2, 6, 1, 7, 0):
        for dc in (1, 0):
            if dz or dc:
                dev = (pop_of(yl, x, (core + dc) % 2), ((z + dz) % NZ) * 2 + yh)
                remote(ref, ref, small_sent.at[1], small_got.at[1], dev).start()

    got(loss1.at[pl.ds(0, 15)], small_got.at[1])
    row = loss1[0]
    for i in range(1, 16):
        row = row + loss1[i]
    loss2[y * NX + x] = row
    ref = loss2.at[y * NX + x]
    for dy in (4, 3, 5, 2, 6, 1, 7, 0):
        for dx in (2, 1, 3, 0):
            if dy or dx:
                remote(ref, ref, small_sent.at[2], small_got.at[2], at_yx((y + dy) % NY, (x + dx) % NX)).start()
    got(leftbuf.at[pl.ds(0, NPOP - 1)], small_got.at[0])
    left_t[...] = leftbuf[...].reshape(MEMBERS, KB).astype(jnp.float32).T

    got(loss2.at[pl.ds(0, 31)], small_got.at[2])

    losses = []
    for q in range(NYL):
        row = loss2[q * NX]
        for i in range(1, NX):
            row = row + loss2[q * NX + i]
        for i in range(NX):
            row = row + loss2[(NYL + q) * NX + i]
        losses.append(row / (LEN * D))
    mean = jnp.sum(losses[0] + losses[1] + losses[2] + losses[3]) / MEMBERS
    squares = [row * row for row in losses]
    spread = jnp.sum(squares[0] + squares[1] + squares[2] + squares[3]) / MEMBERS - mean * mean
    root = jnp.sqrt(jnp.full((1, 128), spread + epsilon, jnp.float32))

    fitness = jnp.concatenate([-(row - mean) / root for row in losses], axis=1)
    weighted = left_t[...] * fitness
    b1 = weighted.astype(jnp.bfloat16)
    b2 = (weighted - b1.astype(jnp.float32)).astype(jnp.bfloat16)
    r = wbuf[:, pl.ds(KB, MEM)].reshape(MEMBERS, COLS)
    total = jnp.dot(jnp.concatenate([b2, b1], axis=0), r, preferred_element_type=jnp.float32)
    total = total[:KB] + total[KB:]
    upd[...] = total * (1.0 / (MEMBERS * sigma_scale))

    left_device(tokbuf, z_sent.at[0])
    left_device(tokbuf.at[pl.ds(0, 2), pl.ds(0, HALF + EXTRA + MEM)], z_sent.at[1])
    left_device(wbuf.at[pl.ds(0, 28)], w_sent)
    @pl.when(middle)
    def _():
        left_device(wbuf.at[pl.ds(0, 5)], y_sent)

    @pl.when(edge)
    def _():
        left_device(wbuf.at[0], y_sent)

    left_device(leftbuf.at[pl.ds(0, NPOP - 1)], small_sent.at[0])
    left_device(loss1.at[pl.ds(0, 15)], small_sent.at[1])
    left_device(loss2.at[pl.ds(0, 31)], small_sent.at[2])


def write_out(hid, upd, hid_hbm, upd_hbm, sem):
    copies = [pltpu.make_async_copy(hid, hid_hbm, sem.at[0]), pltpu.make_async_copy(upd, upd_hbm, sem.at[1])]
    for c in copies:
        c.start()
    for c in copies:
        c.wait()


def per_device(tokens, weight, left, right, target):
    dma = pltpu.SemaphoreType.DMA
    bf, f32 = jnp.bfloat16, jnp.float32
    hidden, update = pl.pallas_call(
        kernel,
        out_shape=(pltpu.VMEM((ROWS, COLS), bf), pltpu.VMEM((KB, COLS), f32)),
        in_specs=[pl.BlockSpec(memory_space=pl.ANY)] * 5,
        out_specs=(pl.BlockSpec(memory_space=pltpu.VMEM), pl.BlockSpec(memory_space=pltpu.VMEM)),
        scratch_shapes=[
            pltpu.VMEM((NTP, TB, COLS), bf),
            pltpu.VMEM((NPOP, WB, COLS), bf),
            pltpu.VMEM((3, HALF, COLS), bf),
            pltpu.VMEM((3, TB - HALF, COLS), bf),
            pltpu.VMEM((ROWS, COLS), f32),
            pltpu.VMEM((ROWS, MEM), f32),
            pltpu.VMEM((ROWS, COLS), bf),
            pltpu.VMEM((NPOP, MEM, KB), bf),
            pltpu.VMEM((KB, MEMBERS), f32),
            pltpu.VMEM((16, 1, 128), f32),
            pltpu.VMEM((32, 1, 128), f32),
            dma((5,)),
            dma((2,)), dma((2, 2, 7)), dma((3,)), dma((3,)),
            dma(()), dma(()), dma((NYL,)), dma((4,)), dma((4,)), dma((4,)),
            dma((3,)), dma((3,)),
            pltpu.SemaphoreType.REGULAR((2,)),
        ],
        compiler_params=pltpu.CompilerParams(
            collective_id=0, has_side_effects=True, vmem_limit_bytes=56 * 1024 * 1024
        ),
    )(tokens, weight, left, right, target)
    return pl.pallas_call(
        write_out,
        out_shape=(jax.ShapeDtypeStruct((ROWS, COLS), bf), jax.ShapeDtypeStruct((KB, COLS), f32)),
        in_specs=[pl.BlockSpec(memory_space=pl.ANY)] * 2,
        out_specs=(pl.BlockSpec(memory_space=pl.ANY), pl.BlockSpec(memory_space=pl.ANY)),
        scratch_shapes=[dma((2,))],
        compiler_params=pltpu.CompilerParams(vmem_limit_bytes=1024 * 1024),
    )(hidden, update)


def solution(mesh):
    return jax.shard_map(
        per_device,
        mesh=mesh,
        in_specs=(P("pop", "tp"), P("pop", "tp"), P("pop", "tp"), P("pop", "tp"), P("pop", "tp")),
        out_specs=(P("pop", "tp"), P("pop", "tp")),
        check_vma=False,
    )
```

```python
import functools

import jax
import jax.numpy as jnp
from jax import lax
from jax.experimental import pallas as pl
from jax.experimental.pallas import tpu as pltpu
from jax.sharding import PartitionSpec as P

D = 8192
LEN = 32
MEMBERS = 512

sigma_scale = 0.5
epsilon = 1e-06

MESH = pl.DeviceIdType.MESH
NX, NY, NYL, NZ = 4, 8, 4, 8
NPOP, NTP = 32, 16
ROWS = 512
COLS = 512
KB = 256
MEM = 16
TB = ROWS + MEM
WB = KB + MEM
LAST = 96
EXTRA = 32
HALF = 256
WHALF = 128


def kernel(
    tok_hbm, w_hbm, left_hbm, right_hbm, tgt_hbm, hid, upd,
    tokbuf, wbuf, relay_a, relay_b, acc, sc, tgt, leftbuf, left_t, loss1, loss2,
    loc, z_sent, zr, rr, mr, y_sent, w_sent, yr, xr, fr, cr, small_sent, small_got,
    entered,
):
    p = lax.axis_index("pop")
    t = lax.axis_index("tp")
    core = p % 2
    x = (p // 2) % NX
    yl = p // (2 * NX)
    z = t // 2
    yh = t % 2
    y = yh * NYL + yl

    def pop_of(yl_, x_, c_):
        return (yl_ * NX + x_) * 2 + c_

    def at_yx(y_, x_):
        return (pop_of(y_ % NYL, x_, core), z * 2 + y_ // NYL)

    def at_y(y_):
        return at_yx(y_ % NY, x)

    def at_x(x_):
        return (pop_of(yl, x_ % NX, core), t)

    def at_z(z_):
        return (p, (z_ % NZ) * 2 + yh)

    other_core = (pop_of(yl, x, 1 - core), t)

    middle = (yl == 1) | (yl == 2)
    edge = jnp.logical_not(middle)

    barrier = pltpu.get_barrier_semaphore()
    near = [at_z(z + 1), at_z(z + NZ - 1), at_y(y + 1), at_y(y + NY - 1), at_x(x + 1), at_x(x + NX - 1), other_core]
    for d in near:
        pl.semaphore_signal(barrier, inc=1, device_id=d, device_id_type=MESH)
    loads = [
        pltpu.make_async_copy(tok_hbm, tokbuf.at[t, pl.ds(0, ROWS)], loc.at[0]),
        pltpu.make_async_copy(left_hbm, tokbuf.at[t, pl.ds(ROWS, MEM)], loc.at[1]),
        pltpu.make_async_copy(w_hbm, wbuf.at[p, pl.ds(0, KB)], loc.at[2]),
        pltpu.make_async_copy(right_hbm, wbuf.at[p, pl.ds(KB, MEM)], loc.at[3]),
        pltpu.make_async_copy(tgt_hbm, tgt, loc.at[4]),
    ]
    for c in loads:
        c.start()

    acc[...] = jnp.zeros_like(acc)
    sc[...] = jnp.zeros_like(sc)
    pl.semaphore_wait(barrier, len(near))

    def remote(src, dst, s, r, dev):
        return pltpu.make_async_remote_copy(
            src_ref=src, dst_ref=dst, send_sem=s, recv_sem=r, device_id=dev, device_id_type=MESH
        )

    def got(ref, sem):
        remote(ref, ref, z_sent.at[0], sem, other_core).wait_recv()

    def left_device(ref, sem):
        remote(ref, ref, sem, mr.at[0], other_core).wait_send()

    def chunk(block, c):
        return tokbuf.at[block, pl.ds(0, HALF)] if c == 0 else tokbuf.at[block, pl.ds(HALF, TB - HALF)]

    def ring_chunk(ring, way, j, dist):
        c = j % 2 if way == 0 else 1 - j % 2
        src_z = z + NZ - dist if way == 0 else z + dist
        block = (src_z % NZ) * 2 + (yh if ring == 0 else 1 - yh)
        if ring == 1 and j >= 5:
            c = 1 - way
            start, rows = (0, LAST) if j == 6 else (LAST, HALF - EXTRA - LAST)
            return tokbuf.at[block, pl.ds(c * HALF + start, rows)]
        return chunk(block, c)

    def zsend(ring, j):
        for way in (0, 1):
            zsend_way(ring, way, j)

    def zsend_way(ring, way, j):
        ref = ring_chunk(ring, way, j, min(j // 2, 2 if ring == 1 else 3))
        dev = at_z(z + 1) if way == 0 else at_z(z + NZ - 1)
        small = ring == 1 and j >= 5
        remote(ref, ref, z_sent.at[1 if small else 0], zr.at[way, ring, j], dev).start()

    def zevent(ring, j):
        for way in (0, 1):
            got(ring_chunk(ring, way, j, min(j // 2, 2 if ring == 1 else 3) + 1), zr.at[way, ring, j])
            if j + 2 < 7 - ring:
                zsend_way(ring, way, j + 2)
            if ring == 1 and j == 3:
                zsend_way(1, way, 6)

    def pieces(n, own_yh, src_z):
        if n < 2:
            block = (src_z % NZ) * 2 + own_yh
            return chunk(block, 0), chunk(block, 1)
        after, before = ((z + 3) % NZ) * 2 + own_yh, ((z + NZ - 3) % NZ) * 2 + own_yh
        return tokbuf.at[after, pl.ds(HALF - EXTRA, EXTRA)], tokbuf.at[before, pl.ds(ROWS - EXTRA, EXTRA + MEM)]

    def relay(n):
        if n < 2:
            return relay_a.at[n], relay_b.at[n]
        return relay_a.at[n, pl.ds(0, EXTRA)], relay_b.at[n, pl.ds(0, EXTRA + MEM)]

    def to_relay(n, src_z):
        for way, ref, buf, dev in zip((0, 1), pieces(n, yh, src_z), relay(n), (at_y(y + 1), at_y(y + NY - 1))):
            remote(ref, buf, z_sent.at[n // 2], rr.at[n], dev).start()

    def from_relay(n, src_z):
        got(tokbuf.at[0] if n < 2 else tokbuf.at[0, pl.ds(0, 2 * EXTRA + MEM)], rr.at[n])
        for way, buf, step in zip((0, 1), relay(n), (3, NY - 3)):
            y_to = (y + step) % NY
            dst = pieces(n, (y_to + NYL) % NY // NYL, src_z)[way]
            remote(buf, dst, z_sent.at[n // 2], mr.at[n], at_y(y_to)).start()

    def mate(n, src_z):
        if n < 2:
            got(tokbuf.at[(src_z % NZ) * 2 + (1 - yh)], mr.at[n])
        else:
            got(tokbuf.at[0, pl.ds(0, 2 * EXTRA + MEM)], mr.at[n])

    def tell(n):
        for dev in (at_y(y + 1), at_y(y + NY - 1)):
            pl.semaphore_signal(entered.at[n], inc=1, device_id=dev, device_id_type=MESH)

    def told(n):
        pl.semaphore_wait(entered.at[n], 2)

    near_y = yl - 1 + 2 * ((3 - yl) // 3)
    far_y = 3 * ((3 - yl) // 2)
    group = (yl, near_y, 6 - yl - near_y - far_y, far_y)

    def wblock(k, dx):
        return wbuf.at[pop_of(group[k], (x + dx + NX) % NX, core)]

    def csend(k, dx):
        ref = wblock(k, dx)
        remote(ref, ref, w_sent, cr.at[k], other_core).start()

    def xsend(k):
        ref = wblock(k, 0)
        remote(ref, ref, w_sent, xr.at[k], at_x(x + 1)).start()
        remote(ref, ref, w_sent, xr.at[k], at_x(x + NX - 1)).start()
        csend(k, 0)

    def ysend(k, up, down):
        ref = wblock(k, 0)

        @pl.when(up)
        def _():
            remote(ref, ref, y_sent, yr.at[group[k]], (pop_of((yl + 1) % NYL, x, core), t)).start()

        @pl.when(down)
        def _():
            remote(ref, ref, y_sent, yr.at[group[k]], (pop_of((yl + NYL - 1) % NYL, x, core), t)).start()

    def yown():
        ysend(0, yl < NYL - 1, yl > 0)

    def ywait(k):
        src = group[k]
        got(wblock(k, 0), yr.at[src])
        ysend(k, (src < yl) & (yl < NYL - 1), (src > yl) & (yl > 0))
        xsend(k)

    lo, hi = pl.ds(0, WHALF), pl.ds(WHALF, WB - WHALF)

    def xwait(k):
        got(wbuf.at[pl.ds(0, 2)], xr.at[k])
        for dx, part, dev in ((-1, lo, at_x(x + 1)), (1, hi, at_x(x + NX - 1))):
            ref = wblock(k, dx).at[part]
            remote(ref, ref, w_sent, fr.at[k], dev).start()
            csend(k, dx)

    def fwait(k):
        got(wblock(k, 2), fr.at[k])
        csend(k, 2)

    def base_rows(block, rows):
        a = tokbuf[block, rows]
        acc[rows, :] += jnp.dot(
            a[:, :KB], wbuf[2 * block, pl.ds(0, KB)], preferred_element_type=jnp.float32
        ) + jnp.dot(a[:, KB:], wbuf[2 * block + 1, pl.ds(0, KB)], preferred_element_type=jnp.float32)

    def score_rows(block, rows):
        sc[rows, :] += lax.dot_general(
            tokbuf[block, rows], tokbuf[block, pl.ds(ROWS, MEM)], (((1,), (1,)), ((), ())),
            preferred_element_type=jnp.float32,
        )

    def left_rows(block):
        for c in (0, 1):
            to = 2 * block + c
            ref = tokbuf.at[block, pl.ds(ROWS, MEM), pl.ds(c * KB, KB)]

            @pl.when(to != p)
            def _():
                remote(ref, leftbuf.at[p], small_sent.at[0], small_got.at[0], (to, t)).start()

            @pl.when(to == p)
            def _():
                leftbuf[p] = ref[...]

    every = pl.ds(0, ROWS)

    def product(block):
        left_rows(block)
        base_rows(block, every)
        score_rows(block, every)

    def at_offset(ring, off):
        return ((z + off) % NZ) * 2 + (yh + ring) % 2

    def group_products(k):
        got(wbuf.at[pl.ds(0, NX)], cr.at[k])

        def body(i, _):
            product((group[k] * 2 + i) * 2 + yh)
            return 0

        lax.fori_loop(0, 2, body, 0)

    def ring_products(first, last):
        def body(i, _):
            odd = i % 2
            product(at_offset(1, (odd * ((i + 1) // 2) + (1 - odd) * (NZ - i // 2)) % NZ))
            return 0

        lax.fori_loop(first, last, body, 0)

    top, low = pl.ds(0, HALF), pl.ds(HALF, ROWS - HALF)

    loads[0].wait()
    loads[1].wait()
    zsend(0, 0)
    zsend(0, 1)
    tell(0)
    loads[2].wait()
    loads[3].wait()
    yown()
    to_relay(0, z)
    xsend(0)
    told(0)
    tell(1)

    zevent(0, 0)
    ywait(1)
    pl.when(middle)(functools.partial(ywait, 2))
    xwait(0)
    zevent(0, 1)
    told(1)
    from_relay(0, z)
    zevent(0, 2)
    zevent(0, 3)
    pl.when(middle)(functools.partial(ywait, 3))
    pl.when(edge)(functools.partial(ywait, 2))
    xwait(1)
    fwait(0)
    zevent(0, 4)
    zevent(0, 5)
    mate(0, z)
    zsend(1, 0)
    zsend(1, 1)
    xwait(2)
    zevent(0, 6)
    to_relay(1, z + 4)
    to_relay(2, z)
    pl.when(edge)(functools.partial(ywait, 3))
    fwait(1)
    zevent(1, 0)
    fwait(2)
    group_products(0)
    from_relay(1, z + 4)
    zevent(1, 1)
    from_relay(2, z)
    xwait(3)
    group_products(1)
    zevent(1, 2)
    group_products(2)
    fwait(3)
    zevent(1, 3)
    group_products(3)
    ring_products(0, 5)
    zevent(1, 4)
    before, after = at_offset(1, NZ - 3), at_offset(1, 3)
    base_rows(before, top)
    base_rows(after, low)
    score_rows(after, low)
    loads[4].wait()
    mate(1, z + 4)
    product(at_offset(1, 4))
    firsts = pl.ds(0, LAST), pl.ds(HALF, LAST)
    rests = pl.ds(LAST, HALF - LAST), pl.ds(HALF + LAST, ROWS - HALF - LAST)
    right_rows = wbuf[p, pl.ds(KB, MEM)].astype(jnp.float32)
    lane = lax.broadcasted_iota(jnp.int32, (LEN, MEM), 1)
    place = lax.broadcasted_iota(jnp.int32, (1, 128), 1)

    def finish(members, mine):
        for m in members:
            rows = pl.ds(m * LEN, LEN)
            s = jnp.sum(jnp.where(lane == m, sc[rows, :], 0.0), axis=1, keepdims=True)
            full = acc[rows, :] + (sigma_scale * s) * right_rows[m : m + 1, :] + tokbuf[t, rows].astype(jnp.float32)
            hid[rows, :] = full.astype(jnp.bfloat16)
            differ = full - tgt[rows, :].astype(jnp.float32)
            total = jnp.sum(jnp.sum(differ * differ, axis=0, keepdims=True), axis=1, keepdims=True)
            mine = mine + jnp.where(place == (p % 8) * MEM + m, total, 0.0)
        return mine

    mate(2, z)
    score_rows(before, top)
    zevent(1, 5)
    for block, seen, scored in ((before, rests[1], (rests[1],)), (after, rests[0], (rests[0],))):
        base_rows(block, seen)
        for rows in scored:
            score_rows(block, rows)
        left_rows(block)
    last_members = [m for m in range(MEM) if m * LEN % HALF < LAST]
    mine = finish([m for m in range(MEM) if m not in last_members], jnp.zeros((1, 128), jnp.float32))
    zevent(1, 6)
    for block, seen in ((before, firsts[1]), (after, firsts[0])):
        base_rows(block, seen)
        score_rows(block, seen)
    loss1[z * 2 + core] = finish(last_members, mine)

    ref = loss1.at[z * 2 + core]
    for dz in (4, 3, 5, 2, 6, 1, 7, 0):
        for dc in (1, 0):
            if dz or dc:
                dev = (pop_of(yl, x, (core + dc) % 2), ((z + dz) % NZ) * 2 + yh)
                remote(ref, ref, small_sent.at[1], small_got.at[1], dev).start()

    got(loss1.at[pl.ds(0, 15)], small_got.at[1])
    row = loss1[0]
    for i in range(1, 16):
        row = row + loss1[i]
    loss2[y * NX + x] = row
    ref = loss2.at[y * NX + x]
    for dy in (4, 3, 5, 2, 6, 1, 7, 0):
        for dx in (2, 1, 3, 0):
            if dy or dx:
                remote(ref, ref, small_sent.at[2], small_got.at[2], at_yx((y + dy) % NY, (x + dx) % NX)).start()
    got(leftbuf.at[pl.ds(0, NPOP - 1)], small_got.at[0])
    left_t[...] = leftbuf[...].reshape(MEMBERS, KB).astype(jnp.float32).T

    got(loss2.at[pl.ds(0, 31)], small_got.at[2])

    losses = []
    for q in range(NYL):
        row = loss2[q * NX]
        for i in range(1, NX):
            row = row + loss2[q * NX + i]
        for i in range(NX):
            row = row + loss2[(NYL + q) * NX + i]
        losses.append(row / (LEN * D))
    mean = jnp.sum(losses[0] + losses[1] + losses[2] + losses[3]) / MEMBERS
    squares = [row * row for row in losses]
    spread = jnp.sum(squares[0] + squares[1] + squares[2] + squares[3]) / MEMBERS - mean * mean
    root = jnp.sqrt(jnp.full((1, 128), spread + epsilon, jnp.float32))

    fitness = jnp.concatenate([-(row - mean) / root for row in losses], axis=1)
    weighted = left_t[...] * fitness
    b1 = weighted.astype(jnp.bfloat16)
    b2 = (weighted - b1.astype(jnp.float32)).astype(jnp.bfloat16)
    r = wbuf[:, pl.ds(KB, MEM)].reshape(MEMBERS, COLS)
    total = jnp.dot(jnp.concatenate([b2, b1], axis=0), r, preferred_element_type=jnp.float32)
    total = total[:KB] + total[KB:]
    upd[...] = total * (1.0 / (MEMBERS * sigma_scale))

    left_device(tokbuf, z_sent.at[0])
    left_device(tokbuf.at[pl.ds(0, 2), pl.ds(0, HALF + EXTRA + MEM)], z_sent.at[1])
    left_device(wbuf.at[pl.ds(0, 28)], w_sent)
    @pl.when(middle)
    def _():
        left_device(wbuf.at[pl.ds(0, 5)], y_sent)

    @pl.when(edge)
    def _():
        left_device(wbuf.at[0], y_sent)

    left_device(leftbuf.at[pl.ds(0, NPOP - 1)], small_sent.at[0])
    left_device(loss1.at[pl.ds(0, 15)], small_sent.at[1])
    left_device(loss2.at[pl.ds(0, 31)], small_sent.at[2])


def write_out(hid, upd, hid_hbm, upd_hbm, sem):
    for i, (src, dst) in enumerate(((upd, upd_hbm), (hid, hid_hbm))):
        rows = src.shape[0] // 4
        for n in range(4):
            part = pl.ds(n * rows, rows)
            pltpu.make_async_copy(src.at[part], dst.at[part], sem.at[i]).start()
    pltpu.make_async_copy(upd, upd_hbm, sem.at[0]).wait()
    pltpu.make_async_copy(hid, hid_hbm, sem.at[1]).wait()


def per_device(tokens, weight, left, right, target):
    dma = pltpu.SemaphoreType.DMA
    bf, f32 = jnp.bfloat16, jnp.float32
    hidden, update = pl.pallas_call(
        kernel,
        out_shape=(pltpu.VMEM((ROWS, COLS), bf), pltpu.VMEM((KB, COLS), f32)),
        in_specs=[pl.BlockSpec(memory_space=pl.ANY)] * 5,
        out_specs=(pl.BlockSpec(memory_space=pltpu.VMEM), pl.BlockSpec(memory_space=pltpu.VMEM)),
        scratch_shapes=[
            pltpu.VMEM((NTP, TB, COLS), bf),
            pltpu.VMEM((NPOP, WB, COLS), bf),
            pltpu.VMEM((3, HALF, COLS), bf),
            pltpu.VMEM((3, TB - HALF, COLS), bf),
            pltpu.VMEM((ROWS, COLS), f32),
            pltpu.VMEM((ROWS, MEM), f32),
            pltpu.VMEM((ROWS, COLS), bf),
            pltpu.VMEM((NPOP, MEM, KB), bf),
            pltpu.VMEM((KB, MEMBERS), f32),
            pltpu.VMEM((16, 1, 128), f32),
            pltpu.VMEM((32, 1, 128), f32),
            dma((5,)),
            dma((2,)), dma((2, 2, 7)), dma((3,)), dma((3,)),
            dma(()), dma(()), dma((NYL,)), dma((4,)), dma((4,)), dma((4,)),
            dma((3,)), dma((3,)),
            pltpu.SemaphoreType.REGULAR((2,)),
        ],
        compiler_params=pltpu.CompilerParams(
            collective_id=0, has_side_effects=True, vmem_limit_bytes=56 * 1024 * 1024
        ),
    )(tokens, weight, left, right, target)
    return pl.pallas_call(
        write_out,
        out_shape=(jax.ShapeDtypeStruct((ROWS, COLS), bf), jax.ShapeDtypeStruct((KB, COLS), f32)),
        in_specs=[pl.BlockSpec(memory_space=pl.ANY)] * 2,
        out_specs=(pl.BlockSpec(memory_space=pl.ANY), pl.BlockSpec(memory_space=pl.ANY)),
        scratch_shapes=[dma((2,))],
        compiler_params=pltpu.CompilerParams(vmem_limit_bytes=1024 * 1024),
    )(hidden, update)


def solution(mesh):
    return jax.shard_map(
        per_device,
        mesh=mesh,
        in_specs=(P("pop", "tp"), P("pop", "tp"), P("pop", "tp"), P("pop", "tp"), P("pop", "tp")),
        out_specs=(P("pop", "tp"), P("pop", "tp")),
        check_vma=False,
    )
```
